256 devices in a mesh: stream: 64 (over x, z, y_hi), span: 4 (over y_lo, core).
Axes of the slice: x: 4, y: 4 (y_hi: 2, y_lo: 2; y = y_hi * 2 + y_lo), z: 8, core: 2. Of those that a mesh axis runs over, the one named last changes fastest.
Arguments:
- state: float32 [2560, 8, 625], P('stream', 'span'), may hold values from -0.25 to 2.5, as said below
- direction: float32 [2560, 8, 625], P('stream', 'span'), may hold values from -6 to 6
- metric: float32 [2560, 8, 3], P('stream', 'span'), may hold values from 1 to 4
- face_source: int32 [2560, 4], P('stream'), may hold values from -1 to 225, as said below
- send_rows: int32 [64, 2, 33], P('stream'), may hold values from 0 to 159, as said below
Outputs:
- residual: float32 [2560, 8, 625], P('stream', 'span')
- basis_next: float32 [2560, 8, 625], P('stream', 'span')
- krylov: float32 [3], replicated
The draws below stay inside these ranges and needn't reach their ends.
Inputs may be any that keep to these rules, and one draw needn't show every extreme that they name: `state`: conserved variables from density 0.75 to 1.25, flow-wise velocity 0.1 to 0.5, other velocities -0.2 to 0.2, pressure 0.5 to 0.9, so pressure and temperature are positive. `face_source`: the plane is a grid of columns of 32 cells, numbered column by column, partition d owning cells d * 40 to (d + 1) * 40 - 1 in a random local order; flow-wise faces wrap around. Every face neighbour lies in the same or an adjacent partition; -1 stands exactly on the lower face of the lowest and the upper face of the highest row; indices into received blocks point at used slots. `send_rows`: at most 33 faces per neighbouring pair, and some pair uses all 33; slots beyond a pair's count hold 0; the order of slots is the order in which the receiver's face_source refers to them.
All inputs are finite; a program needn't handle non-finite values.
Results may differ from the reference program's by a relative error of at most 0.0003.
Values sent between devices are 32-bit elements.
A program may use at most 128 MiB of HBM per device.

```python
import math
import jax
import jax.numpy as jnp
import numpy as np
from jax import lax

COLUMNS = 40
WALL_ROWS = 32
NODES = 125
VARS = 5
SLOTS = 33
PLANE = 2560
LAYERS = 8
N_STREAM = 64


GAMMA_RATIO = 1.4


def draw_state(key, part):
    noise_shape = (PLANE, LAYERS, 5, NODES)
    noise = jnp.clip(0.4 * jax.random.normal(key, noise_shape, jnp.float32), -1.0, 1.0)
    density = 1.0 + 0.25 * noise[:, :, 0]
    flow_speed = 0.3 + 0.2 * noise[:, :, 1]
    normal_speed = 0.2 * noise[:, :, 2]
    span_speed = 0.2 * noise[:, :, 3]
    pressure = 0.7 + 0.2 * noise[:, :, 4]
    kinetic = 0.5 * density * (flow_speed * flow_speed + normal_speed * normal_speed + span_speed * span_speed)
    energy = pressure / (GAMMA_RATIO - 1.0) + kinetic
    stacked = jnp.stack([density, density * flow_speed, density * normal_speed, density * span_speed, energy], axis=2)
    return stacked.reshape(PLANE, LAYERS, 5 * NODES)


def mesh_tables(key):
    devices = N_STREAM
    cell_ids = jnp.arange(PLANE, dtype=jnp.int32)
    owner_part = cell_ids // COLUMNS
    position = cell_ids % COLUMNS
    part_keys = jax.random.split(jax.random.fold_in(key, 17), devices)
    orders = jax.vmap(lambda single: jax.random.permutation(single, COLUMNS))(part_keys).astype(jnp.int32)
    local_column = orders[owner_part, position]
    column_count = PLANE // WALL_ROWS
    flow_column = cell_ids // WALL_ROWS
    wall_row = cell_ids % WALL_ROWS
    neighbor = jnp.stack([(flow_column - 1) % column_count * WALL_ROWS + wall_row, (flow_column + 1) % column_count * WALL_ROWS + wall_row, cell_ids - 1, cell_ids + 1], axis=1)
    walled = jnp.stack([wall_row < 0, wall_row < 0, wall_row == 0, wall_row == WALL_ROWS - 1], axis=1)
    neighbor = jnp.where(walled, cell_ids[:, None], neighbor)
    other_owner = neighbor // COLUMNS
    face_ids = jnp.arange(4, dtype=jnp.int32)[None, :]
    to_left = jnp.logical_and(jnp.logical_not(walled), other_owner == (owner_part[:, None] - 1) % devices)
    to_right = jnp.logical_and(jnp.logical_not(walled), other_owner == (owner_part[:, None] + 1) % devices)

    def slots_of(flags):
        flat_flags = flags.reshape(devices, COLUMNS * 4).astype(jnp.int32)
        before = jnp.cumsum(flat_flags, axis=1) - flat_flags
        return before.reshape(PLANE, 4)
    left_slot = slots_of(to_left)
    right_slot = slots_of(to_right)
    own_index = local_column[:, None] * 4 + face_ids
    owners = jnp.broadcast_to(owner_part[:, None], (PLANE, 4))
    send_table = jnp.zeros((devices, 2, SLOTS), jnp.int32)
    send_table = send_table.at[owners, 0, jnp.where(to_left, left_slot, SLOTS)].set(own_index, mode='drop')
    send_table = send_table.at[owners, 1, jnp.where(to_right, right_slot, SLOTS)].set(own_index, mode='drop')
    partner_face = face_ids + 1 - 2 * (face_ids % 2)
    partner_local = local_column[neighbor] * 4 + partner_face
    from_right = COLUMNS * 4 + SLOTS + left_slot[neighbor, partner_face]
    from_left = COLUMNS * 4 + right_slot[neighbor, partner_face]
    source = jnp.where(to_right, from_right, jnp.where(to_left, from_left, partner_local))
    source = jnp.where(walled, -1, source).astype(jnp.int32)
    row_ids = owner_part * COLUMNS + local_column
    source_table = jnp.zeros((PLANE, 4), jnp.int32).at[row_ids].set(source)
    return (source_table, send_table)


def draw_face_source(key, part):
    return mesh_tables(key)[0]


def draw_send_rows(key, part):
    return mesh_tables(key)[1]


def levels(key, shape, pieces, least, high):
    factor_of, own = 1.0, jax.random.fold_in(key, 6)
    for axis_at, shards_of in pieces:
        draws = jnp.exp(jax.random.uniform(jax.random.fold_in(own, axis_at), (shards_of,), jnp.float32, least / len(pieces), high / len(pieces)))
        factor_of = factor_of * jnp.repeat(draws, shape[axis_at] // shards_of).reshape([-1 if axis == axis_at else 1 for axis in range(len(shape))])
    return factor_of


def bell_draw(key, extent, scale, limit, shards=(), held_as=jnp.bfloat16):
    values = scale * jax.random.normal(key, extent, jnp.float32)
    if shards:
        values = values * levels(key, extent, shards, -0.22, 0.18)
    return jnp.clip(values, -limit, limit).astype(held_as)


def setup_inputs(seed: int = 0) -> dict:
    arg_keys = jax.random.split(jax.random.key(seed), 6)
    return {
        "state": draw_state(jax.random.fold_in(arg_keys[5], 71), 0),
        "direction": bell_draw(arg_keys[1], (PLANE, LAYERS, NODES * VARS), 1.0, 6.0, ((0, 64), (1, 4)), jnp.float32),
        "metric": jnp.clip(jnp.exp(math.log(4.0) - 1.3862944 * jax.random.uniform(arg_keys[2], (PLANE, LAYERS, 3), jnp.float32) ** levels(arg_keys[2], (PLANE, LAYERS, 3), ((0, 64), (1, 4)), -0.2, 0.2)), 1.0, 4.0),
        "face_source": draw_face_source(jax.random.fold_in(arg_keys[5], 71), 0),
        "send_rows": draw_send_rows(jax.random.fold_in(arg_keys[5], 71), 0),
    }


GAMMA = 1.4
VISC = 0.01
COND = VISC * GAMMA / ((GAMMA - 1.0) * 0.72)
LIFT = 10.0
EINSUM_FORMS = ('ai,...ijk->...ajk', 'aj,...ijk->...iak', 'ak,...ijk->...ija')

def diff_table():
    spread = math.sqrt(3.0 / 7.0)
    points = np.array([-1.0, -spread, 0.0, spread, 1.0])
    weights = np.array([np.prod([points[row_at] - points[other] for other in range(5) if other != row_at]) for row_at in range(5)])
    matrix = np.zeros((5, 5))
    for row_at in range(5):
        for col_at in range(5):
            if row_at != col_at:
                matrix[row_at, col_at] = weights[row_at] / (weights[col_at] * (points[row_at] - points[col_at]))
        matrix[row_at, row_at] = np.sum([1.0 / (points[row_at] - points[other]) for other in range(5) if other != row_at])
    return matrix

def derivative(field, axis_pick):
    matrix = jnp.asarray(diff_table(), dtype=jnp.float32)
    return jnp.einsum(EINSUM_FORMS[axis_pick], matrix, field, precision=lax.Precision.HIGHEST)

def face_slice(volume, face_index):
    endpoint = 4 * (face_index % 2)
    if face_index < 2:
        return volume[..., endpoint, :, :]
    if face_index < 4:
        return volume[..., :, endpoint, :]
    return volume[..., :, :, endpoint]

def put_face(volume, face_index, values):
    endpoint = 4 * (face_index % 2)
    if face_index < 2:
        return volume.at[..., endpoint, :, :].add(values)
    if face_index < 4:
        return volume.at[..., :, endpoint, :].add(values)
    return volume.at[..., :, :, endpoint].add(values)

def primitive(components):
    density = components[0]
    velocity = [components[1] / density, components[2] / density, components[3] / density]
    kinetic = 0.5 * (components[1] * velocity[0] + components[2] * velocity[1] + components[3] * velocity[2])
    pressure = (GAMMA - 1.0) * (components[4] - kinetic)
    return (velocity, pressure, pressure / density)

def inviscid(components, axis_pick):
    velocity, pressure, temper = primitive(components)
    normal_speed = velocity[axis_pick]
    result = [components[1 + axis_pick]]
    for member in range(3):
        flux_term = components[1 + member] * normal_speed
        if member == axis_pick:
            flux_term = flux_term + pressure
        result.append(flux_term)
    result.append((components[4] + pressure) * normal_speed)
    return result

def viscous(components, gradients, axis_pick):
    velocity, pressure, temper = primitive(components)
    divergence = gradients[0][0] + gradients[1][1] + gradients[2][2]
    stresses = []
    for member in range(3):
        stress = gradients[axis_pick][member] + gradients[member][axis_pick]
        if member == axis_pick:
            stress = stress - 2.0 / 3.0 * divergence
        stresses.append(VISC * stress)
    energy = stresses[0] * velocity[0] + stresses[1] * velocity[1] + stresses[2] * velocity[2] + COND * gradients[axis_pick][3]
    return [jnp.zeros_like(energy)] + stresses + [energy]

def wave_square(components):
    velocity, pressure, temper = primitive(components)
    return velocity[0] * velocity[0] + velocity[1] * velocity[1] + velocity[2] * velocity[2] + GAMMA * temper

def lifted_gradient(volume, outside, scales):
    components = [volume[..., member, :, :, :] for member in range(5)]
    velocity, pressure, temper = primitive(components)
    fields = velocity + [temper]
    outer_fields = []
    for face_index in range(6):
        outer_parts = [outside[face_index][..., member, :, :] for member in range(5)]
        outer_velocity, outer_pressure, outer_temper = primitive(outer_parts)
        outer_fields.append(outer_velocity + [outer_temper])
    gradients = []
    for axis_pick in range(3):
        factor = scales[..., axis_pick][..., None, None, None]
        grad_row = []
        for field_index in range(4):
            accumulated = derivative(fields[field_index], axis_pick)
            for upper_side in range(2):
                face_index = 2 * axis_pick + upper_side
                normal_sign = 2.0 * upper_side - 1.0
                trace_jump = outer_fields[face_index][field_index] - face_slice(fields[field_index], face_index)
                accumulated = put_face(accumulated, face_index, 0.5 * LIFT * normal_sign * trace_jump)
            grad_row.append(factor * accumulated)
        gradients.append(grad_row)
    return gradients

def own_viscous_faces(volume, gradients):
    components = [volume[..., member, :, :, :] for member in range(5)]
    result = []
    for face_index in range(6):
        face_parts = [face_slice(piece, face_index) for piece in components]
        face_grads = [[face_slice(entry, face_index) for entry in grad_row] for grad_row in gradients]
        result.append(jnp.stack(viscous(face_parts, face_grads, face_index // 2), axis=-3))
    return result

def residual_terms(volume, outside, gradients, visc_outside, scales, walls):
    components = [volume[..., member, :, :, :] for member in range(5)]
    totals = [jnp.zeros_like(components[0]) for member in range(5)]
    for axis_pick in range(3):
        factor = scales[..., axis_pick][..., None, None, None]
        convect = inviscid(components, axis_pick)
        diffuse = viscous(components, gradients, axis_pick)
        accumulated = [derivative(convect[member] - diffuse[member], axis_pick) for member in range(5)]
        for upper_side in range(2):
            face_index = 2 * axis_pick + upper_side
            normal_sign = 2.0 * upper_side - 1.0
            inner_parts = [face_slice(piece, face_index) for piece in components]
            outer_parts = [outside[face_index][..., member, :, :] for member in range(5)]
            outer_flux = inviscid(outer_parts, axis_pick)
            speed = jnp.sqrt(0.5 * (wave_square(inner_parts) + wave_square(outer_parts)))
            for member in range(5):
                inner_visc = face_slice(diffuse[member], face_index)
                outer_visc = visc_outside[face_index][..., member, :, :]
                if walls[face_index] is not None:
                    outer_visc = jnp.where(walls[face_index], inner_visc, outer_visc)
                surface = normal_sign * 0.5 * (outer_flux[member] - face_slice(convect[member], face_index)) - 0.5 * speed * (outer_parts[member] - inner_parts[member]) - normal_sign * 0.5 * (outer_visc - inner_visc)
                accumulated[member] = put_face(accumulated[member], face_index, LIFT * surface)
        totals = [totals[member] + factor * accumulated[member] for member in range(5)]
    return jnp.stack(totals, axis=-4)

def wall_masks(face_source):
    masks = [None, None, None, None, None, None]
    for face_index in (2, 3):
        masks[face_index] = (face_source[:, face_index] < 0)[:, None, None, None]
    return masks

def mirrored(face_trace):
    flips = 2.0 * (jnp.arange(5) % 4 == 0).astype(jnp.float32) - 1.0
    return face_trace * flips[:, None, None]

def pack_faces(volume):
    lead_shape = volume.shape[:2] + (-1,)
    return jnp.stack([face_slice(volume, face_index).reshape(lead_shape) for face_index in range(6)], axis=1)

def stack_faces(face_list):
    lead_shape = face_list[0].shape[:2] + (-1,)
    return jnp.stack([entry.reshape(lead_shape) for entry in face_list], axis=1)

def send_buffers(table, send_rows):
    picked = jnp.take(table, send_rows.reshape(-1), axis=0)
    return picked.reshape((2, send_rows.shape[2]) + table.shape[1:])

def pick_outside(table, received, face_source):
    whole = jnp.concatenate([table, received[0], received[3]], axis=0)
    picked = jnp.take(whole, jnp.maximum(face_source, 0).reshape(-1), axis=0)
    return picked.reshape(face_source.shape + table.shape[1:])

def split_traces(outside, upper_half, trailing):
    half_width = outside[0].shape[-1] // 2
    offset = half_width * upper_half
    return [entry[..., offset:offset + half_width].reshape(entry.shape[:-1] + trailing) for entry in outside]

def with_walls(outside, own_volume, walls):
    result = []
    for face_index in range(6):
        face_trace = outside[face_index]
        if walls[face_index] is not None:
            face_trace = jnp.where(walls[face_index][..., None], mirrored(face_slice(own_volume, face_index)), face_trace)
        result.append(face_trace)
    return result

def plane_reference(own_faces, face_source, send_rows):
    devices = send_rows.shape[0]
    table = own_faces[:, :4].reshape((devices, -1) + own_faces.shape[2:])
    buffers = jax.vmap(send_buffers)(table, send_rows[:, None])
    received = jnp.stack([jnp.roll(buffers[:, 1], 1, axis=0), buffers[:, 0], buffers[:, 1], jnp.roll(buffers[:, 0], -1, axis=0)], axis=1)
    plane = jax.vmap(pick_outside)(table, received, face_source.reshape(devices, -1, 4))
    plane = plane.reshape((-1,) + plane.shape[2:])
    return [plane[:, 0], plane[:, 1], plane[:, 2], plane[:, 3]]

def reference(state, direction, metric, face_source, send_rows):
    element = (5, 5, 5, 5)
    primal = jnp.moveaxis(state.reshape((PLANE, LAYERS) + element), 1, 0)[:, :, None]
    tangent = jnp.moveaxis(direction.reshape((PLANE, LAYERS) + element), 1, 0)[:, :, None]
    scales = jnp.moveaxis(metric, 1, 0)[:, :, None]
    walls = wall_masks(face_source)
    lead_shape = (LAYERS, PLANE, 1, -1)
    bottoms = jnp.concatenate([face_slice(primal, 4).reshape(lead_shape), face_slice(tangent, 4).reshape(lead_shape)], axis=-1)
    tops = jnp.concatenate([face_slice(primal, 5).reshape(lead_shape), face_slice(tangent, 5).reshape(lead_shape)], axis=-1)
    below_states = jnp.roll(tops, 1, axis=0)
    above_states = jnp.roll(bottoms, -1, axis=0)

    def first_section(volume_p, volume_t, scales_layer, below, above):
        own_states = jnp.concatenate([pack_faces(volume_p), pack_faces(volume_t)], axis=-1)
        outside = plane_reference(own_states, face_source, send_rows) + [below, above]
        outside_p = with_walls(split_traces(outside, 0, (5, 5, 5)), volume_p, walls)
        outside_t = with_walls(split_traces(outside, 1, (5, 5, 5)), volume_t, walls)
        grad_p, grad_t = jax.jvp(lambda volume, outer_side: lifted_gradient(volume, outer_side, scales_layer), (volume_p, outside_p), (volume_t, outside_t))
        return (outside_p, outside_t, grad_p, grad_t)

    def visc_section(inputs):
        volume_p, volume_t, scales_layer, below, above = inputs
        outside_p, outside_t, grad_p, grad_t = first_section(volume_p, volume_t, scales_layer, below, above)
        visc_p, visc_t = jax.jvp(own_viscous_faces, (volume_p, grad_p), (volume_t, grad_t))
        return jnp.concatenate([stack_faces(visc_p), stack_faces(visc_t)], axis=-1)
    own_visc = lax.map(visc_section, (primal, tangent, scales, below_states, above_states))
    visc_below = jnp.roll(own_visc[:, :, 5], 1, axis=0)
    visc_above = jnp.roll(own_visc[:, :, 4], -1, axis=0)

    def final_section(inputs):
        volume_p, volume_t, scales_layer, below, above, visc_own, visc_low, visc_high = inputs
        outside_p, outside_t, grad_p, grad_t = first_section(volume_p, volume_t, scales_layer, below, above)
        visc_out = plane_reference(visc_own, face_source, send_rows) + [visc_low, visc_high]
        visc_p = split_traces(visc_out, 0, (5, 5, 5))
        visc_t = split_traces(visc_out, 1, (5, 5, 5))
        return jax.jvp(lambda volume, outer_side, gradients, visc_side: residual_terms(volume, outer_side, gradients, visc_side, scales_layer, walls), (volume_p, outside_p, grad_p, visc_p), (volume_t, outside_t, grad_t, visc_t))
    res_p, res_t = lax.map(final_section, (primal, tangent, scales, below_states, above_states, own_visc, visc_below, visc_above))
    residual = jnp.moveaxis(res_p[:, :, 0], 0, 1).reshape(state.shape)
    product = jnp.moveaxis(res_t[:, :, 0], 0, 1).reshape(state.shape)
    total = float(state.size)
    coefficient = jnp.sum(direction * product) / total
    remainder = product - coefficient * direction
    beta = jnp.sqrt(jnp.sum(remainder * remainder) / total)
    norm_value = jnp.sqrt(jnp.sum(residual * residual) / total)
    return (residual, remainder / beta, jnp.stack([coefficient, beta, norm_value]))
```

```python
import math

import jax
import jax.numpy as jnp
import numpy as np
from jax import lax
from jax.experimental import pallas as pl
from jax.experimental.pallas import tpu as pltpu
from jax.sharding import PartitionSpec as P

MESH = pl.DeviceIdType.MESH
F32 = jnp.float32
BF16 = jnp.bfloat16

GAMMA = 1.4
VISC = 0.01
COND = VISC * GAMMA / ((GAMMA - 1.0) * 0.72)

COLS = 40
LAYERS = 2
ROWS = COLS * LAYERS
SLOTS = 33
CHUNK = 8
STRIDES = (25, 5, 1)
GROUP = 16


def diff_table():
    spread = math.sqrt(3.0 / 7.0)
    points = np.array([-1.0, -spread, 0.0, spread, 1.0])
    weights = np.array(
        [
            np.prod([points[row_at] - points[other] for other in range(5) if other != row_at])
            for row_at in range(5)
        ]
    )
    matrix = np.zeros((5, 5))
    for row_at in range(5):
        for col_at in range(5):
            if row_at != col_at:
                matrix[row_at, col_at] = weights[row_at] / (
                    weights[col_at] * (points[row_at] - points[col_at])
                )
        matrix[row_at, row_at] = np.sum(
            [1.0 / (points[row_at] - points[other]) for other in range(5) if other != row_at]
        )
    return matrix


def operator_table():
    line = diff_table()
    line[0, 0] += 5.0
    line[4, 4] -= 5.0
    eye = np.eye(5)
    full = np.zeros((128, 384), np.float32)
    for axis in range(3):
        parts = [eye, eye, eye]
        parts[axis] = line
        volume = np.kron(np.kron(parts[0], parts[1]), parts[2])
        full[:125, axis * 128 : axis * 128 + 125] = volume.T
    high = full.astype(jnp.bfloat16)
    low = (full - high.astype(np.float32)).astype(jnp.bfloat16)
    return np.concatenate([high, high, low], axis=0)


def lane_table():
    table = np.zeros((8, 128), np.float32)
    lanes = np.arange(125)
    for axis, stride in enumerate(STRIDES):
        digit = (lanes // stride) % 5
        table[axis] = 9.0
        table[axis, :125] = digit
        table[3 + axis, :125] = 5.0 * (digit == 4) - 5.0 * (digit == 0)
    table[6, :125] = 1.0
    return table


def roll(value, shift):
    shift %= 128
    return value if shift == 0 else pltpu.roll(value, shift, 1)


def split2(value):
    high = value.astype(BF16)
    return high, (value - high.astype(F32)).astype(BF16)


def split3(value):
    high = value.astype(BF16)
    rest = value - high.astype(F32)
    mid = rest.astype(BF16)
    return high, mid, (rest - mid.astype(F32)).astype(BF16)


def dot(a, b):
    return lax.dot_general(a, b, (((1,), (0,)), ((), ())), preferred_element_type=F32)


def primitive(u, du):
    r = 1.0 / u[0]
    v = [u[1 + i] * r for i in range(3)]
    dv = [(du[1 + i] - v[i] * du[0]) * r for i in range(3)]
    vm = u[1] * v[0] + u[2] * v[1] + u[3] * v[2]
    p = (GAMMA - 1.0) * (u[4] - 0.5 * vm)
    vdm = v[0] * du[1] + v[1] * du[2] + v[2] * du[3]
    vv = v[0] * v[0] + v[1] * v[1] + v[2] * v[2]
    dp = (GAMMA - 1.0) * (du[4] - vdm + 0.5 * vv * du[0])
    t = p * r
    dt = (dp - t * du[0]) * r
    s2 = vv + GAMMA * t
    ds2 = 2.0 * (v[0] * dv[0] + v[1] * dv[1] + v[2] * dv[2]) + GAMMA * dt
    return v, p, t, dv, dp, dt, s2, ds2


def inviscid(u, du, v, p, dv, dp, axis):
    flux = [u[1 + axis]]
    tangent = [du[1 + axis]]
    for i in range(3):
        f = u[1 + i] * v[axis]
        df = du[1 + i] * v[axis] + u[1 + i] * dv[axis]
        if i == axis:
            f = f + p
            df = df + dp
        flux.append(f)
        tangent.append(df)
    flux.append((u[4] + p) * v[axis])
    tangent.append((du[4] + dp) * v[axis] + (u[4] + p) * dv[axis])
    return flux, tangent


def stress(q):
    third = (2.0 / 3.0) * (q[0][0] + q[1][1] + q[2][2])
    tau = [[None] * 3 for _ in range(3)]
    for a in range(3):
        tau[a][a] = VISC * (2.0 * q[a][a] - third)
        for b in range(a + 1, 3):
            tau[a][b] = tau[b][a] = VISC * (q[a][b] + q[b][a])
    return tau


def kernel(
    state_ref,
    dir_ref,
    met_ref,
    fs_ref,
    sr_ref,
    op_ref,
    lane_ref,
    res_ref,
    bas_ref,
    kry_ref,
    x_s,
    u_s,
    w_s,
    c_s,
    m_s,
    fy_s,
    oo_s,
    or_s,
    tab_s,
    zp_s,
    zv_s,
    sb1,
    sb2,
    rx1,
    rx2,
    zs1,
    zs2,
    rz1,
    rz2,
    g_s,
    q_s,
    o_s,
    po_s,
    v_s,
    h_s,
    r_s,
    rs_s,
    y_s,
    acc_s,
    pt_s,
    pb_s,
    ar_a,
    ar_b,
    xs_send,
    xs_recv,
    as_send,
    as_recv,
    bs_send,
    bs_recv,
):
    s = lax.axis_index("stream")
    p = lax.axis_index("span")
    n_s, n_p = 64, 4
    s_lo, s_hi = lax.rem(s + n_s - 1, n_s), lax.rem(s + 1, n_s)
    p_lo, p_hi = lax.rem(p + n_p - 1, n_p), lax.rem(p + 1, n_p)
    quad = 4 * (s // 4)
    mine_a = p * 4 + lax.rem(s, 4)
    mine_b = s // 4

    def peer_a(k):
        j = lax.rem(mine_a + k, GROUP)
        return {"stream": quad + lax.rem(j, 4), "span": j // 4}, j

    def peer_b(k):
        j = lax.rem(mine_b + k, GROUP)
        return {"stream": 4 * j + lax.rem(s, 4), "span": p}, j

    barrier = pltpu.get_barrier_semaphore()

    def greet(target):
        pl.semaphore_signal(barrier, inc=1, device_id=target, device_id_type=MESH)

    greet({"stream": s_lo, "span": p})
    greet({"stream": s_hi, "span": p})
    greet({"stream": s, "span": p_lo})
    greet({"stream": s, "span": p_hi})
    for k in range(1, GROUP):
        greet(peer_a(k)[0])
        greet(peer_b(k)[0])

    lane = lax.broadcasted_iota(jnp.int32, (CHUNK, 128), 1)
    digit = [jnp.broadcast_to(lane_ref[a : a + 1, :], (CHUNK, 128)) for a in range(3)]
    sgn = [jnp.broadcast_to(lane_ref[3 + a : 4 + a, :], (CHUNK, 128)) for a in range(3)]
    node = lane < 125

    for l in range(LAYERS):
        x_s[0, l * COLS : (l + 1) * COLS, 0:625] = state_ref[:, l, :]
        x_s[1, l * COLS : (l + 1) * COLS, 0:625] = dir_ref[:, l, :]

    def pack(fields, axis, upper):
        base = 4 if upper else 0
        acc = None
        for v, field in enumerate(fields):
            moved = roll(field, (v - base) * STRIDES[axis])
            acc = moved if acc is None else jnp.where(digit[axis] == float(v), moved, acc)
        return acc

    def pack_faces(fields, pt, l, rc):
        col = (pt * LAYERS + l) * 128
        for f in range(4):
            tab_s[pl.ds(f * COLS + rc, CHUNK), col : col + 128] = pack(fields, f // 2, f % 2)
        for f in range(2):
            zp_s[f, l, pt, pl.ds(rc, CHUNK), :] = pack(fields, 2, f)

    def each_chunk(body):
        for l in range(LAYERS):

            def step(i, carry, l=l):
                rc = pl.multiple_of(i * CHUNK, CHUNK)
                body(l, rc, pl.multiple_of(l * COLS + rc, CHUNK))
                return carry

            lax.fori_loop(0, COLS // CHUNK, step, 0)

    def first(l, rc, row):
        for pt in range(2):
            tiles = [x_s[pt, pl.ds(row, CHUNK), 128 * t : 128 * t + 128] for t in range(5)]
            fields = []
            for v in range(5):
                value = roll(tiles[v], 3 * v)
                if v:
                    value = jnp.where(lane < 3 * v, roll(tiles[v - 1], 3 * v), value)
                idle = 1.0 if pt == 0 and v in (0, 4) else 0.0
                value = jnp.where(node, value, idle)
                u_s[pt * 5 + v, pl.ds(row, CHUNK), :] = value
                fields.append(value)
            pack_faces(fields, pt, l, rc)

    each_chunk(first)

    eye = lax.broadcasted_iota(jnp.int32, (COLS, COLS), 0) == lax.broadcasted_iota(
        jnp.int32, (COLS, COLS), 1
    )

    def column(row):
        return jnp.sum(
            jnp.where(eye, jnp.broadcast_to(row, (COLS, COLS)), 0.0), axis=1, keepdims=True
        )

    k_own = lax.broadcasted_iota(jnp.int32, (COLS, 160), 1)
    g_own = (
        jnp.where(k_own >= 40, 159, 0)
        + jnp.where(k_own >= 80, 159, 0)
        + jnp.where(k_own >= 120, 159, 0)
    )
    own_id = (4 * k_own - g_own).astype(F32)
    k_rec = lax.broadcasted_iota(jnp.int32, (COLS, 80), 1)
    rec_id = jnp.where(
        k_rec < SLOTS,
        k_rec + 160,
        jnp.where((k_rec >= COLS) & (k_rec < COLS + SLOTS), k_rec + 153, -5),
    ).astype(F32)
    sends = []
    for side in range(2):
        ids = sr_ref[side : side + 1, :].astype(F32)
        slot = lax.broadcasted_iota(jnp.int32, (COLS, SLOTS), 0) == lax.broadcasted_iota(
            jnp.int32, (COLS, SLOTS), 1
        )
        col = jnp.sum(
            jnp.where(slot, jnp.broadcast_to(ids, (COLS, SLOTS)), 0.0), axis=1, keepdims=True
        )
        sends.append(jnp.where(col == own_id, 1.0, 0.0))
    send_hot = jnp.concatenate(sends, axis=0).astype(BF16)

    def remote(src, dst, sem, target):
        return pltpu.make_async_remote_copy(
            src_ref=src,
            dst_ref=dst,
            send_sem=xs_send.at[sem],
            recv_sem=xs_recv.at[sem],
            device_id=target,
            device_id_type=MESH,
        )

    def exchange(sb, rx, zs, rz, base):
        return [
            remote(zs.at[0], rz.at[1], base, {"stream": s, "span": p_lo}),
            remote(zs.at[1], rz.at[0], base + 1, {"stream": s, "span": p_hi}),
            remote(sb.at[pl.ds(0, COLS)], rx.at[pl.ds(COLS, COLS)], base + 2, {"stream": s_lo, "span": p}),
            remote(sb.at[pl.ds(COLS, COLS)], rx.at[pl.ds(0, COLS)], base + 3, {"stream": s_hi, "span": p}),
        ]

    def send(sb, rx, faces, zs, rz, base, wait):
        table = split3(tab_s[...])
        sb[...] = dot(send_hot, table[0]) + (dot(send_hot, table[1]) + dot(send_hot, table[2]))
        zs[0] = faces[0, 0]
        zs[1] = faces[1, LAYERS - 1]
        if wait:
            pl.semaphore_wait(barrier, 4 + 2 * (GROUP - 1))
        copies = exchange(sb, rx, zs, rz, base)
        for copy in copies:
            copy.start()
        return copies, table

    copies1, table = send(sb1, rx1, zp_s, zs1, rz1, 0, True)

    for f in range(4):
        col = column(fs_ref[f : f + 1, :].astype(F32))
        oo_s[f * COLS : (f + 1) * COLS, :] = jnp.where(col == own_id, 1.0, 0.0).astype(BF16)
        or_s[f * COLS : (f + 1) * COLS, :] = jnp.where(col == rec_id, 1.0, 0.0).astype(BF16)
        if f >= 2:
            fy_s[f - 2] = jnp.broadcast_to(col, (COLS, 128))
    for a in range(3):
        for l in range(LAYERS):
            m_s[a, l * COLS : (l + 1) * COLS, :] = jnp.broadcast_to(
                column(met_ref[a, l : l + 1, :]), (COLS, 128)
            )

    def own_gather(table):
        hot = oo_s[...]
        g_s[...] = dot(hot, table[0]) + (dot(hot, table[1]) + dot(hot, table[2]))

    def far_gather(rx):
        hot = or_s[...]
        table = split3(rx[...])
        g_s[...] += dot(hot, table[0]) + (dot(hot, table[1]) + dot(hot, table[2]))

    own_gather(table)

    def second(l, rc, row):
        u = [u_s[v, pl.ds(row, CHUNK), :] for v in range(10)]
        v, pr, t, dv, dp, dt, s2, ds2 = primitive(u[:5], u[5:])
        for i, value in enumerate(v + [t] + dv + [dt]):
            w_s[pl.ds(pl.multiple_of(i * ROWS + row, CHUNK), CHUNK), :] = value
        for i, value in enumerate([pr, dp, s2, ds2]):
            c_s[i, pl.ds(row, CHUNK), :] = value

    each_chunk(second)
    high, low = split2(w_s[...])
    q_s[...] = dot(jnp.concatenate([high, low, high], axis=1), op_ref[...])

    for copy in copies1:
        copy.wait()
    far_gather(rx1)

    def face_masks(rc):
        masks = []
        for axis in range(3):
            lower, upper = digit[axis] == 0.0, digit[axis] == 4.0
            if axis == 1:
                lower = lower & (fy_s[0, pl.ds(rc, CHUNK), :] >= 0.0)
                upper = upper & (fy_s[1, pl.ds(rc, CHUNK), :] >= 0.0)
            masks.append((lower, upper))
        return masks

    def packed_pair(axis, pt, l, rc, faces, rz):
        if axis < 2:
            col = (pt * LAYERS + l) * 128
            return [
                g_s[pl.ds(f * COLS + rc, CHUNK), col : col + 128] for f in (2 * axis, 2 * axis + 1)
            ]
        below = rz[0, pt, pl.ds(rc, CHUNK), :] if l == 0 else faces[1, l - 1, pt, pl.ds(rc, CHUNK), :]
        above = (
            rz[1, pt, pl.ds(rc, CHUNK), :]
            if l == LAYERS - 1
            else faces[0, l + 1, pt, pl.ds(rc, CHUNK), :]
        )
        return [below, above]

    def unpack(pair, v, axis, masks, inside):
        stride = STRIDES[axis]
        upper = jnp.where(masks[axis][1], roll(pair[1], (4 - v) * stride), inside)
        return jnp.where(masks[axis][0], roll(pair[0], -v * stride), upper)

    def third(l, rc, row):
        masks = face_masks(rc)
        here = pl.ds(row, CHUNK)
        u = [u_s[v, here, :] for v in range(10)]
        inside = [-value if v % 5 in (1, 2, 3) else value for v, value in enumerate(u)]
        q = [[], []]
        for axis in range(3):
            out = []
            for pt in range(2):
                pair = packed_pair(axis, pt, l, rc, zp_s, rz1)
                for v in range(5):
                    out.append(unpack(pair, v, axis, masks, inside[pt * 5 + v]))
            for i, value in enumerate(out):
                o_s[axis, i, here, :] = value
            v, pr, t, dv, dp, dt, s2, ds2 = primitive(out[:5], out[5:])
            for i, value in enumerate(v + [pr, s2] + dv + [dp, ds2]):
                po_s[axis, i, here, :] = value
            factor = m_s[axis, here, :]
            for i, value in enumerate(v + [t] + dv + [dt]):
                volume = q_s[pl.ds(pl.multiple_of(i * ROWS + row, CHUNK), CHUNK), axis * 128 : axis * 128 + 128]
                q[i // 4].append(factor * (volume + sgn[axis] * value))
        w = [w_s[pl.ds(pl.multiple_of(i * ROWS + row, CHUNK), CHUNK), :] for i in range(8)]
        tau, dtau = [stress([q[pt][4 * a : 4 * a + 3] for a in range(3)]) for pt in range(2)]
        col = (l * 128, (LAYERS + l) * 128)
        for a in range(3):
            energy = COND * q[0][4 * a + 3]
            tangent = COND * q[1][4 * a + 3]
            for b in range(3):
                energy = energy + w[b] * tau[a][b]
                tangent = tangent + (w[4 + b] * tau[a][b] + w[b] * dtau[a][b])
            for pt, flux in enumerate((tau[a] + [energy], dtau[a] + [tangent])):
                for i, value in enumerate(flux):
                    v_s[a, pt * 4 + i, here, :] = value
                for up in range(2):
                    if a < 2:
                        tab_s[pl.ds((2 * a + up) * COLS + rc, CHUNK), col[pt] : col[pt] + 128] = pack(flux, a, up)
                    else:
                        zv_s[up, l, pt, pl.ds(rc, CHUNK), :] = pack(flux, a, up)

    each_chunk(third)
    copies2, table = send(sb2, rx2, zv_s, zs2, rz2, 4, False)

    own_gather(table)

    def fourth(l, rc, row):
        here = pl.ds(row, CHUNK)
        u = [u_s[v, here, :] for v in range(10)]
        w = [w_s[pl.ds(pl.multiple_of(i * ROWS + row, CHUNK), CHUNK), :] for i in range(8)]
        pr, dp, s2, ds2 = [c_s[i, here, :] for i in range(4)]
        total = [None] * 10
        for a in range(3):
            factor = m_s[a, here, :]
            flux, tangent = inviscid(u[:5], u[5:], w[:3], pr, w[4:7], dp, a)
            for pt, values in enumerate((flux, tangent)):
                for i, value in enumerate(values):
                    if i:
                        value = value - v_s[a, pt * 4 + i - 1, here, :]
                    at = pl.multiple_of((pt * 5 + i) * ROWS + row, CHUNK)
                    h_s[a, pl.ds(at, CHUNK), :] = factor * value
            out = [o_s[a, i, here, :] for i in range(10)]
            po = [po_s[a, i, here, :] for i in range(10)]
            flux, tangent = inviscid(out[:5], out[5:], po[:3], po[3], po[5:8], po[8], a)
            speed = jnp.sqrt(0.5 * (s2 + po[4]))
            dspeed = 0.25 * (ds2 + po[9]) / speed
            side = factor * sgn[a]
            drag = jnp.abs(side)
            for i in range(5):
                jump = out[i] - u[i]
                term = side * flux[i] - drag * (speed * jump)
                dterm = side * tangent[i] - drag * (dspeed * jump + speed * (out[5 + i] - u[5 + i]))
                total[i] = term if a == 0 else total[i] + term
                total[5 + i] = dterm if a == 0 else total[5 + i] + dterm
        for i in range(10):
            rs_s[i, here, :] = total[i]

    each_chunk(fourth)
    volume = None
    for a in range(3):
        high, low = split2(h_s[a])
        part = dot(jnp.concatenate([high, low, high], axis=1), op_ref[:, a * 128 : a * 128 + 128])
        volume = part if a == 0 else volume + part
    r_s[...] = volume

    for copy in copies2:
        copy.wait()
    far_gather(rx2)

    pt_s[...] = jnp.zeros((8, 128), F32)

    def fifth(l, rc, row):
        masks = face_masks(rc)
        here = pl.ds(row, CHUNK)
        total = [
            r_s[pl.ds(pl.multiple_of(i * ROWS + row, CHUNK), CHUNK), :] + rs_s[i, here, :]
            for i in range(10)
        ]
        for a in range(3):
            side = m_s[a, here, :] * sgn[a]
            for pt in range(2):
                pair = packed_pair(a, pt, l, rc, zv_s, rz2)
                for i in range(4):
                    value = unpack(pair, i, a, masks, v_s[a, pt * 4 + i, here, :])
                    total[pt * 5 + 1 + i] = total[pt * 5 + 1 + i] - side * value
        total = [jnp.where(node, value, 0.0) for value in total]
        du = [u_s[5 + i, here, :] for i in range(5)]
        sums = [None] * 4
        for i in range(5):
            terms = (
                du[i] * total[5 + i],
                du[i] * du[i],
                total[i] * total[i],
                total[5 + i] * total[5 + i],
            )
            sums = [term if i == 0 else old + term for old, term in zip(sums, terms)]
        for i in range(4):
            acc_s[i] += sums[i]
        for pt in range(2):
            fields = total[5 * pt : 5 * pt + 5]
            for t in range(5):
                value = roll(fields[t], -3 * t)
                if t < 4:
                    value = jnp.where(lane < 125 - 3 * t, value, roll(fields[t + 1], 125 - 3 * t))
                y_s[pt, here, 128 * t : 128 * t + 128] = value

    acc_s[...] = jnp.zeros((4, CHUNK, 128), F32)
    each_chunk(fifth)
    for i in range(4):
        pt_s[i : i + 1, :] = jnp.sum(acc_s[i], axis=0, keepdims=True)

    def stage(src, dst, mine, peer, send_sem, recv_sem):
        dst[mine] = src[...]

        def copy_to(k):
            target, j = peer(k)
            return pltpu.make_async_remote_copy(
                src_ref=src,
                dst_ref=dst.at[mine],
                send_sem=send_sem.at[k],
                recv_sem=recv_sem.at[k],
                device_id=target,
                device_id_type=MESH,
            )

        for k in range(1, GROUP):
            copy_to(k).start()
        return copy_to

    def collect(copy_to, dst):
        for k in range(1, GROUP):
            copy_to(k).wait()
        return jnp.sum(dst[...], axis=0)

    first_stage = stage(pt_s, ar_a, mine_a, peer_a, as_send, as_recv)
    for l in range(LAYERS):
        res_ref[:, l, :] = y_s[0, l * COLS : (l + 1) * COLS, 0:625]
    pb_s[...] = collect(first_stage, ar_a)
    second_stage = stage(pb_s, ar_b, mine_b, peer_b, bs_send, bs_recv)
    sums = collect(second_stage, ar_b)
    dp_sum, dd_sum, rr_sum, pp_sum = [
        jnp.sum(sums[i : i + 1, :], axis=1, keepdims=True) for i in range(4)
    ]
    count = 1.0 / float(n_s * n_p * ROWS * 625)
    coefficient = dp_sum * count
    beta = jnp.sqrt(
        (pp_sum - 2.0 * coefficient * dp_sum + coefficient * coefficient * dd_sum) * count
    )
    norm = jnp.sqrt(rr_sum * count)
    at = lax.broadcasted_iota(jnp.int32, (1, 128), 1)
    kry_ref[...] = jnp.where(at == 0, coefficient, jnp.where(at == 1, beta, norm))
    scale = 1.0 / beta
    for l in range(LAYERS):
        part = pl.ds(l * COLS, COLS)
        value = (y_s[1, part, :] - coefficient * x_s[1, part, :]) * scale
        bas_ref[:, l, :] = value[:, 0:625]


def local(state, direction, metric, face_source, send_rows):
    vmem = pl.BlockSpec(memory_space=pltpu.VMEM)
    shapes = [
        ((2, ROWS, 640), F32),
        ((10, ROWS, 128), F32),
        ((8 * ROWS, 128), F32),
        ((4, ROWS, 128), F32),
        ((3, ROWS, 128), F32),
        ((2, COLS, 128), F32),
        ((160, 160), BF16),
        ((160, 80), BF16),
        ((160, 512), F32),
        ((2, LAYERS, 2, COLS, 128), F32),
        ((2, LAYERS, 2, COLS, 128), F32),
        ((80, 512), F32),
        ((80, 512), F32),
        ((80, 512), F32),
        ((80, 512), F32),
        ((2, 2, COLS, 128), F32),
        ((2, 2, COLS, 128), F32),
        ((2, 2, COLS, 128), F32),
        ((2, 2, COLS, 128), F32),
        ((160, 512), F32),
        ((8 * ROWS, 384), F32),
        ((3, 10, ROWS, 128), F32),
        ((3, 10, ROWS, 128), F32),
        ((3, 8, ROWS, 128), F32),
        ((3, 10 * ROWS, 128), F32),
        ((10 * ROWS, 128), F32),
        ((10, ROWS, 128), F32),
        ((2, ROWS, 640), F32),
        ((4, CHUNK, 128), F32),
        ((8, 128), F32),
        ((8, 128), F32),
        ((GROUP, 8, 128), F32),
        ((GROUP, 8, 128), F32),
    ]
    res, bas, kry = pl.pallas_call(
        kernel,
        out_shape=(
            jax.ShapeDtypeStruct(state.shape, F32),
            jax.ShapeDtypeStruct(state.shape, F32),
            jax.ShapeDtypeStruct((1, 128), F32),
        ),
        in_specs=[vmem] * 7,
        out_specs=(vmem, vmem, vmem),
        scratch_shapes=[pltpu.VMEM(shape, dtype) for shape, dtype in shapes]
        + [pltpu.SemaphoreType.DMA((8,))] * 2
        + [pltpu.SemaphoreType.DMA((GROUP,))] * 4,
        compiler_params=pltpu.CompilerParams(
            collective_id=0, has_side_effects=True, vmem_limit_bytes=48 * 1024 * 1024
        ),
        name="hill",
    )(
        state,
        direction,
        jnp.transpose(metric, (2, 1, 0)),
        jnp.transpose(face_source),
        send_rows[0],
        jnp.asarray(operator_table()),
        jnp.asarray(lane_table()),
    )
    return res, bas, kry[0, :3]


def solution(mesh):
    in_specs = (
        P("stream", "span", None),
        P("stream", "span", None),
        P("stream", "span", None),
        P("stream", None),
        P("stream", None, None),
    )
    out_specs = (P("stream", "span", None), P("stream", "span", None), P())
    return jax.shard_map(local, mesh=mesh, in_specs=in_specs, out_specs=out_specs, check_vma=False)
```

```python
import math

import jax
import jax.numpy as jnp
import numpy as np
from jax import lax
from jax.experimental import pallas as pl
from jax.experimental.pallas import tpu as pltpu
from jax.sharding import PartitionSpec as P

MESH = pl.DeviceIdType.MESH
F32 = jnp.float32
BF16 = jnp.bfloat16

GAMMA = 1.4
VISC = 0.01
COND = VISC * GAMMA / ((GAMMA - 1.0) * 0.72)

COLS = 40
LAYERS = 2
ROWS = COLS * LAYERS
SLOTS = 33
SENT = 40
CHUNK = 8
STRIDES = (25, 5, 1)
N_X, N_Z, N_SPAN = 4, 8, 4
PLANE = 2 * N_X * N_SPAN


def diff_table():
    spread = math.sqrt(3.0 / 7.0)
    points = np.array([-1.0, -spread, 0.0, spread, 1.0])
    weights = np.array(
        [
            np.prod([points[row_at] - points[other] for other in range(5) if other != row_at])
            for row_at in range(5)
        ]
    )
    matrix = np.zeros((5, 5))
    for row_at in range(5):
        for col_at in range(5):
            if row_at != col_at:
                matrix[row_at, col_at] = weights[row_at] / (
                    weights[col_at] * (points[row_at] - points[col_at])
                )
        matrix[row_at, row_at] = np.sum(
            [1.0 / (points[row_at] - points[other]) for other in range(5) if other != row_at]
        )
    return matrix


def operator_table():
    line = diff_table()
    line[0, 0] += 5.0
    line[4, 4] -= 5.0
    eye = np.eye(5)
    full = np.zeros((128, 384), np.float32)
    for axis in range(3):
        parts = [eye, eye, eye]
        parts[axis] = line
        volume = np.kron(np.kron(parts[0], parts[1]), parts[2])
        full[:125, axis * 128 : axis * 128 + 125] = volume.T
    high = full.astype(jnp.bfloat16)
    low = (full - high.astype(np.float32)).astype(jnp.bfloat16)
    return np.concatenate([high, high, low], axis=0)


def lane_table():
    table = np.zeros((16, 128), np.float32)
    lanes = np.arange(125)
    for axis, stride in enumerate(STRIDES):
        digit = (lanes // stride) % 5
        table[axis] = 9.0
        table[axis, :125] = digit
        table[3 + axis, :125] = 5.0 * (digit == 4) - 5.0 * (digit == 0)
        table[6 + axis] = 9.0
        for var in range(5):
            table[6 + axis, (lanes[digit == 4] + var * stride) % 128] = var
    return table


def roll(value, shift):
    shift %= 128
    return value if shift == 0 else pltpu.roll(value, shift, 1)


def split2(value):
    high = value.astype(BF16)
    return high, (value - high.astype(F32)).astype(BF16)


def split3(value):
    high = value.astype(BF16)
    rest = value - high.astype(F32)
    mid = rest.astype(BF16)
    return high, mid, (rest - mid.astype(F32)).astype(BF16)


def dot(a, b):
    return lax.dot_general(a, b, (((1,), (0,)), ((), ())), preferred_element_type=F32)


def primitive(u, du):
    r = 1.0 / u[0]
    v = [u[1 + i] * r for i in range(3)]
    dv = [(du[1 + i] - v[i] * du[0]) * r for i in range(3)]
    vm = u[1] * v[0] + u[2] * v[1] + u[3] * v[2]
    p = (GAMMA - 1.0) * (u[4] - 0.5 * vm)
    vdm = v[0] * du[1] + v[1] * du[2] + v[2] * du[3]
    vv = v[0] * v[0] + v[1] * v[1] + v[2] * v[2]
    dp = (GAMMA - 1.0) * (du[4] - vdm + 0.5 * vv * du[0])
    t = p * r
    dt = (dp - t * du[0]) * r
    s2 = vv + GAMMA * t
    ds2 = 2.0 * (v[0] * dv[0] + v[1] * dv[1] + v[2] * dv[2]) + GAMMA * dt
    return v, p, t, dv, dp, dt, s2, ds2


def inviscid(u, du, v, p, dv, dp, axis):
    flux = [u[1 + axis]]
    tangent = [du[1 + axis]]
    for i in range(3):
        f = u[1 + i] * v[axis]
        df = du[1 + i] * v[axis] + u[1 + i] * dv[axis]
        if i == axis:
            f = f + p
            df = df + dp
        flux.append(f)
        tangent.append(df)
    flux.append((u[4] + p) * v[axis])
    tangent.append((du[4] + dp) * v[axis] + (u[4] + p) * dv[axis])
    return flux, tangent


def stress(q):
    third = (2.0 / 3.0) * (q[0][0] + q[1][1] + q[2][2])
    tau = [[None] * 3 for _ in range(3)]
    for a in range(3):
        tau[a][a] = VISC * (2.0 * q[a][a] - third)
        for b in range(a + 1, 3):
            tau[a][b] = tau[b][a] = VISC * (q[a][b] + q[b][a])
    return tau


def kernel(
    state_in,
    dir_in,
    met_in,
    fs_in,
    sr_in,
    op_in,
    lane_in,
    res_ref,
    bas_ref,
    kry_ref,
    state_ref,
    dir_ref,
    met_ref,
    fs_ref,
    sr_ref,
    op_ref,
    lane_ref,
    x_s,
    u_s,
    w_s,
    c_s,
    m_s,
    fy_s,
    oo_s,
    or_s,
    so_s,
    tab_s,
    zp_s,
    zv_s,
    sb1,
    sb2,
    rx1,
    rx2,
    rz1,
    rz2,
    g_s,
    q_s,
    o_s,
    po_s,
    v_s,
    h_s,
    r_s,
    rs_s,
    y_s,
    x_out,
    acc_s,
    pt_s,
    pb_s,
    ar_a,
    ar_b,
    xs_send,
    xs_recv,
    sum_sem,
    in_sem,
):
    loads = [
        pltpu.make_async_copy(src, dst, in_sem.at[i])
        for i, (src, dst) in enumerate(
            (
                (state_in, state_ref),
                (dir_in, dir_ref),
                (lane_in, lane_ref),
                (sr_in, sr_ref),
                (fs_in, fs_ref),
                (met_in, met_ref),
                (op_in, op_ref),
            )
        )
    ]
    for load in loads:
        load.start()

    s = lax.axis_index("stream")
    p = lax.axis_index("span")
    n_s = 2 * N_X * N_Z
    s_lo, s_hi = lax.rem(s + n_s - 1, n_s), lax.rem(s + 1, n_s)
    p_lo, p_hi = lax.rem(p + N_SPAN - 1, N_SPAN), lax.rem(p + 1, N_SPAN)
    core = lax.rem(p, 2)
    x_at, z_at, y_hi, y_lo = s // (2 * N_Z), lax.rem(s // 2, N_Z), lax.rem(s, 2), p // 2
    chip = 4 * x_at + 2 * y_hi + y_lo
    mine = 2 * chip + core

    def plane_peer(j):
        return {
            "stream": (j // 8) * (2 * N_Z) + 2 * z_at + lax.rem(j // 4, 2),
            "span": lax.rem(j, 4),
        }

    def column_peer(z, c):
        return {"stream": x_at * (2 * N_Z) + 2 * z + y_hi, "span": 2 * y_lo + c}

    barrier = pltpu.get_barrier_semaphore()

    def greet(target):
        pl.semaphore_signal(barrier, inc=1, device_id=target, device_id_type=MESH)

    greet({"stream": s_lo, "span": p})
    greet({"stream": s_hi, "span": p})
    greet({"stream": s, "span": p_lo})
    greet({"stream": s, "span": p_hi})

    for k in range(1, N_Z):
        greet(column_peer(lax.rem(z_at + k, N_Z), 1))

    @pl.when(core == 1)
    def _():
        for k in range(1, PLANE):
            greet(plane_peer(lax.rem(mine + k, PLANE)))

    @pl.when(core == 0)
    def _():
        greet(column_peer(z_at, 1))

    for load in loads[:3]:
        load.wait()
    lane = lax.broadcasted_iota(jnp.int32, (CHUNK, 128), 1)
    rows = [jnp.broadcast_to(lane_ref[a : a + 1, :], (CHUNK, 128)) for a in range(9)]
    digit, sgn, over = rows[:3], rows[3:6], rows[6:]
    node = lane < 125

    for l in range(LAYERS):
        x_s[0, l * COLS : (l + 1) * COLS, 0:625] = state_ref[:, l, :]
        x_s[1, l * COLS : (l + 1) * COLS, 0:625] = dir_ref[:, l, :]

    def pack(fields, axis):
        stride = STRIDES[axis]
        lower = upper = fields[0]
        for v, field in enumerate(fields):
            if v:
                moved = roll(field, v * stride)
                lower = jnp.where(digit[axis] == float(v), moved, lower)
                upper = jnp.where(over[axis] == float(v), moved, upper)
        return roll(lower, 4 * stride), roll(upper, -4 * stride)

    def pack_axis(fields, axis, pt, l, rc, faces):
        for up, value in enumerate(pack(fields, axis)):
            if axis < 2:
                at = (2 * axis + up) * COLS + rc
                tab_s[l, pl.ds(at, CHUNK), pt * 128 : pt * 128 + 128] = value
            else:
                faces[up, l, pt, pl.ds(rc, CHUNK), :] = value

    def layer_loop(body, l):
        def step(i, carry):
            rc = pl.multiple_of(i * CHUNK, CHUNK)
            body(l, rc, pl.multiple_of(l * COLS + rc, CHUNK))
            return carry

        lax.fori_loop(0, COLS // CHUNK, step, 0, unroll=COLS // CHUNK)

    def first(l, rc, row):
        for pt in range(2):
            tiles = [x_s[pt, pl.ds(row, CHUNK), 128 * t : 128 * t + 128] for t in range(5)]
            fields = []
            for v in range(5):
                value = roll(tiles[v], 3 * v)
                if v:
                    value = jnp.where(lane < 3 * v, roll(tiles[v - 1], 3 * v), value)
                idle = 1.0 if pt == 0 and v in (0, 4) else 0.0
                value = jnp.where(node, value, idle)
                u_s[pt * 5 + v, pl.ds(row, CHUNK), :] = value
                fields.append(value)
            for axis in range(3):
                pack_axis(fields, axis, pt, l, rc, zp_s)

    def remote(src, dst, sem, target):
        return pltpu.make_async_remote_copy(
            src_ref=src,
            dst_ref=dst,
            send_sem=xs_send.at[sem],
            recv_sem=xs_recv.at[sem],
            device_id=target,
            device_id_type=MESH,
        )

    def z_copies(faces, rz, base):
        return [
            remote(faces.at[0, 0], rz.at[1], base, {"stream": s, "span": p_lo}),
            remote(faces.at[1, LAYERS - 1], rz.at[0], base + 1, {"stream": s, "span": p_hi}),
        ]

    def xy_copies(sb, rx, l, base):
        lower, upper = pl.ds(0, SENT), pl.ds(COLS, SENT)
        return [
            remote(sb.at[l, lower], rx.at[l, upper], base + 2 + 2 * l, {"stream": s_lo, "span": p}),
            remote(sb.at[l, upper], rx.at[l, lower], base + 3 + 2 * l, {"stream": s_hi, "span": p}),
        ]

    def start(copies):
        for copy in copies:
            copy.start()

    def wait(copies):
        for copy in copies:
            copy.wait()

    def gather(hot, table):
        parts = split3(table)
        return dot(hot, parts[0]) + (dot(hot, parts[1]) + dot(hot, parts[2]))

    def fill(sb, l):
        sb[l] = gather(so_s[...], tab_s[l])

    with jax.named_scope("first0"):
        layer_loop(first, 0)

    for load in loads[3:]:
        load.wait()
    eye = lax.broadcasted_iota(jnp.int32, (COLS, COLS), 0) == lax.broadcasted_iota(
        jnp.int32, (COLS, COLS), 1
    )

    def column(row):
        return jnp.sum(
            jnp.where(eye, jnp.broadcast_to(row, (COLS, COLS)), 0.0), axis=1, keepdims=True
        )

    k_own = lax.broadcasted_iota(jnp.int32, (COLS, 160), 1)
    g_own = (
        jnp.where(k_own >= 40, 159, 0)
        + jnp.where(k_own >= 80, 159, 0)
        + jnp.where(k_own >= 120, 159, 0)
    )
    own_id = (4 * k_own - g_own).astype(F32)
    k_rec = lax.broadcasted_iota(jnp.int32, (COLS, 80), 1)
    rec_id = jnp.where(
        k_rec < SLOTS,
        k_rec + 160,
        jnp.where((k_rec >= COLS) & (k_rec < COLS + SLOTS), k_rec + 153, -5),
    ).astype(F32)
    slot = lax.broadcasted_iota(jnp.int32, (COLS, SLOTS), 0) == lax.broadcasted_iota(
        jnp.int32, (COLS, SLOTS), 1
    )
    for side in range(2):
        ids = sr_ref[side : side + 1, :].astype(F32)
        col = jnp.sum(
            jnp.where(slot, jnp.broadcast_to(ids, (COLS, SLOTS)), 0.0), axis=1, keepdims=True
        )
        so_s[side * COLS : (side + 1) * COLS, :] = jnp.where(col == own_id, 1.0, 0.0).astype(BF16)

    round1 = [xy_copies(sb1, rx1, l, 0) for l in range(LAYERS)]
    round1_z = z_copies(zp_s, rz1, 0)
    round2 = [xy_copies(sb2, rx2, l, 6) for l in range(LAYERS)]
    round2_z = z_copies(zv_s, rz2, 6)

    fill(sb1, 0)
    with jax.named_scope("barrier"):
        pl.semaphore_wait(barrier, 4 + 16 + 14 * core)
    start(round1[0])
    with jax.named_scope("first1"):
        layer_loop(first, 1)
        start(round1_z)
        fill(sb1, 1)
        start(round1[1])

    for f in range(4):
        col = column(fs_ref[f : f + 1, :].astype(F32))
        oo_s[f * COLS : (f + 1) * COLS, :] = jnp.where(col == own_id, 1.0, 0.0).astype(BF16)
        or_s[f * COLS : (f + 1) * COLS, :] = jnp.where(col == rec_id, 1.0, 0.0).astype(BF16)
        if f >= 2:
            fy_s[f - 2] = jnp.broadcast_to(col, (COLS, 128))
    for a in range(3):
        for l in range(LAYERS):
            m_s[a, l * COLS : (l + 1) * COLS, :] = jnp.broadcast_to(
                column(met_ref[a, l : l + 1, :]), (COLS, 128)
            )

    def own_gather(l):
        g_s[l] = gather(oo_s[...], tab_s[l])

    def far_gather(rx, l):
        table = rx[l]
        if SENT < COLS:
            at = lax.broadcasted_iota(jnp.int32, (2 * COLS, 256), 0)
            used = (at < SLOTS) | ((at >= COLS) & (at < COLS + SLOTS))
            table = jnp.where(used, table, 0.0)
        g_s[l] += gather(or_s[...], table)

    def second(l, rc, row):
        u = [u_s[v, pl.ds(row, CHUNK), :] for v in range(10)]
        v, pr, t, dv, dp, dt, s2, ds2 = primitive(u[:5], u[5:])
        for i, value in enumerate(v + [t] + dv + [dt]):
            w_s[pl.ds(pl.multiple_of(i * ROWS + row, CHUNK), CHUNK), :] = value
        for i, value in enumerate([pr, dp, s2, ds2]):
            c_s[i, pl.ds(row, CHUNK), :] = value

    for l in range(LAYERS):
        layer_loop(second, l)
    high, low = split2(w_s[...])
    q_s[...] = dot(jnp.concatenate([high, low, high], axis=1), op_ref[...])
    for l in range(LAYERS):
        own_gather(l)

    def face_masks(rc):
        masks = []
        for axis in range(3):
            lower, upper = digit[axis] == 0.0, digit[axis] == 4.0
            if axis == 1:
                lower = lower & (fy_s[0, pl.ds(rc, CHUNK), :] >= 0.0)
                upper = upper & (fy_s[1, pl.ds(rc, CHUNK), :] >= 0.0)
            masks.append(lower | upper)
        return masks

    def packed_pair(axis, pt, l, rc, faces, rz):
        here = pl.ds(rc, CHUNK)
        if axis < 2:
            return [
                g_s[l, pl.ds(f * COLS + rc, CHUNK), pt * 128 : pt * 128 + 128]
                for f in (2 * axis, 2 * axis + 1)
            ]
        below = rz[0, pt, here, :] if l == 0 else faces[1, l - 1, pt, here, :]
        above = rz[1, pt, here, :] if l == LAYERS - 1 else faces[0, l + 1, pt, here, :]
        return [below, above]

    def unpack(pair, v, axis, masks, inside):
        mixed = jnp.where(digit[axis] == float(v), pair[0], pair[1])
        return jnp.where(masks[axis], roll(mixed, -v * STRIDES[axis]), inside)

    def third(l, rc, row):
        masks = face_masks(rc)
        here = pl.ds(row, CHUNK)
        u = [u_s[v, here, :] for v in range(10)]
        inside = [-value if v % 5 in (1, 2, 3) else value for v, value in enumerate(u)]
        q = [[], []]
        for axis in range(3):
            out = []
            for pt in range(2):
                pair = packed_pair(axis, pt, l, rc, zp_s, rz1)
                for v in range(5):
                    out.append(unpack(pair, v, axis, masks, inside[pt * 5 + v]))
            for i, value in enumerate(out):
                o_s[axis, i, here, :] = value
            v, pr, t, dv, dp, dt, s2, ds2 = primitive(out[:5], out[5:])
            for i, value in enumerate(v + [pr, s2] + dv + [dp, ds2]):
                po_s[axis, i, here, :] = value
            factor = m_s[axis, here, :]
            for i, value in enumerate(v + [t] + dv + [dt]):
                at = pl.multiple_of(i * ROWS + row, CHUNK)
                volume = q_s[pl.ds(at, CHUNK), axis * 128 : axis * 128 + 128]
                q[i // 4].append(factor * (volume + sgn[axis] * value))
        w = [w_s[pl.ds(pl.multiple_of(i * ROWS + row, CHUNK), CHUNK), :] for i in range(8)]
        tau, dtau = [stress([q[pt][4 * a : 4 * a + 3] for a in range(3)]) for pt in range(2)]
        for a in range(3):
            energy = COND * q[0][4 * a + 3]
            tangent = COND * q[1][4 * a + 3]
            for b in range(3):
                energy = energy + w[b] * tau[a][b]
                tangent = tangent + (w[4 + b] * tau[a][b] + w[b] * dtau[a][b])
            for pt, flux in enumerate((tau[a] + [energy], dtau[a] + [tangent])):
                for i, value in enumerate(flux):
                    v_s[a, pt * 4 + i, here, :] = value
                pack_axis(flux, a, pt, l, rc, zv_s)

    with jax.named_scope("wait1z"):
        wait(round1_z)
    for l in range(LAYERS):
        with jax.named_scope("wait1"):
            wait(round1[l])
        with jax.named_scope("third"):
            far_gather(rx1, l)
            layer_loop(third, l)
            start(round2_z[l : l + 1])
            fill(sb2, l)
            start(round2[l])

    def fourth(l, rc, row):
        here = pl.ds(row, CHUNK)
        u = [u_s[v, here, :] for v in range(10)]
        w = [w_s[pl.ds(pl.multiple_of(i * ROWS + row, CHUNK), CHUNK), :] for i in range(8)]
        pr, dp, s2, ds2 = [c_s[i, here, :] for i in range(4)]
        total = [None] * 10
        for a in range(3):
            factor = m_s[a, here, :]
            flux, tangent = inviscid(u[:5], u[5:], w[:3], pr, w[4:7], dp, a)
            for pt, values in enumerate((flux, tangent)):
                for i, value in enumerate(values):
                    if i:
                        value = value - v_s[a, pt * 4 + i - 1, here, :]
                    at = pl.multiple_of((pt * 5 + i) * ROWS + row, CHUNK)
                    h_s[a, pl.ds(at, CHUNK), :] = factor * value
            out = [o_s[a, i, here, :] for i in range(10)]
            po = [po_s[a, i, here, :] for i in range(10)]
            flux, tangent = inviscid(out[:5], out[5:], po[:3], po[3], po[5:8], po[8], a)
            speed = jnp.sqrt(0.5 * (s2 + po[4]))
            dspeed = 0.25 * (ds2 + po[9]) / speed
            side = factor * sgn[a]
            drag = jnp.abs(side)
            for i in range(5):
                jump = out[i] - u[i]
                term = side * flux[i] - drag * (speed * jump)
                dterm = side * tangent[i] - drag * (dspeed * jump + speed * (out[5 + i] - u[5 + i]))
                total[i] = term if a == 0 else total[i] + term
                total[5 + i] = dterm if a == 0 else total[5 + i] + dterm
        for i in range(10):
            rs_s[i, here, :] = total[i]

    with jax.named_scope("fourth"):
        for l in range(LAYERS):
            own_gather(l)
            layer_loop(fourth, l)
    with jax.named_scope("resmm"):
        volume = None
        for a in range(3):
            high, low = split2(h_s[a])
            part = dot(jnp.concatenate([high, low, high], axis=1), op_ref[:, a * 128 : a * 128 + 128])
            volume = part if a == 0 else volume + part
        r_s[...] = volume
        acc_s[...] = jnp.zeros((4, CHUNK, 128), F32)

    def fifth(l, rc, row):
        masks = face_masks(rc)
        here = pl.ds(row, CHUNK)
        total = [
            r_s[pl.ds(pl.multiple_of(i * ROWS + row, CHUNK), CHUNK), :] + rs_s[i, here, :]
            for i in range(10)
        ]
        for a in range(3):
            side = m_s[a, here, :] * sgn[a]
            for pt in range(2):
                pair = packed_pair(a, pt, l, rc, zv_s, rz2)
                for i in range(4):
                    value = unpack(pair, i, a, masks, v_s[a, pt * 4 + i, here, :])
                    total[pt * 5 + 1 + i] = total[pt * 5 + 1 + i] - side * value
        total = [jnp.where(node, value, 0.0) for value in total]
        du = [u_s[5 + i, here, :] for i in range(5)]
        sums = [None] * 4
        for i in range(5):
            terms = (
                du[i] * total[5 + i],
                du[i] * du[i],
                total[i] * total[i],
                total[5 + i] * total[5 + i],
            )
            sums = [term if i == 0 else old + term for old, term in zip(sums, terms)]
        for i in range(4):
            acc_s[i] += sums[i]
        for i in range(10):
            y_s[i, here, :] = total[i]

    with jax.named_scope("wait2z"):
        wait(round2_z)
    for l in range(LAYERS):
        with jax.named_scope("wait2"):
            wait(round2[l])
        with jax.named_scope("fifth"):
            far_gather(rx2, l)
            layer_loop(fifth, l)

    at = lax.broadcasted_iota(jnp.int32, (1, 128), 1)
    own = [jnp.sum(acc_s[i], axis=(0, 1), keepdims=True) for i in range(4)]
    own = jnp.where(at == 0, own[0], jnp.where(at == 1, own[1], jnp.where(at == 2, own[2], own[3])))
    pt_s[...] = own

    def to_plane(k):
        return pltpu.make_async_remote_copy(
            src_ref=pt_s,
            dst_ref=ar_a.at[mine],
            send_sem=sum_sem.at[0],
            recv_sem=sum_sem.at[1],
            device_id=plane_peer(2 * lax.rem(chip + k, PLANE // 2) + 1),
            device_id_type=MESH,
        )

    def to_column(k, c):
        return pltpu.make_async_remote_copy(
            src_ref=pb_s,
            dst_ref=ar_b.at[z_at],
            send_sem=sum_sem.at[2],
            recv_sem=sum_sem.at[3],
            device_id=column_peer(lax.rem(z_at + k, N_Z), c),
            device_id_type=MESH,
        )

    def drain(buffer, count, sem):
        part = buffer.at[pl.ds(0, count)]
        pltpu.make_async_copy(part, part, sum_sem.at[sem]).wait()

    for k in range(1, PLANE // 2):
        to_plane(k).start()

    @pl.when(core == 0)
    def _():
        to_plane(0).start()

    @pl.when(core == 1)
    def _():
        ar_a[mine] = own

    def tile(fields, t):
        value = roll(fields[t], -3 * t)
        if t < 4:
            value = jnp.where(lane < 125 - 3 * t, value, roll(fields[t + 1], 125 - 3 * t))
        return value

    def sixth(l, rc, row):
        here = pl.ds(row, CHUNK)
        fields = [y_s[i, here, :] for i in range(10)]
        for pt in range(2):
            for t in range(5):
                x_out[pt, here, 128 * t : 128 * t + 128] = tile(fields[5 * pt : 5 * pt + 5], t)

    with jax.named_scope("sixth"):
        for l in range(LAYERS):
            layer_loop(sixth, l)
        for l in range(LAYERS):
            res_ref[:, l, :] = x_out[0, l * COLS : (l + 1) * COLS, 0:625]

    with jax.named_scope("sums"):

        @pl.when(core == 1)
        def _():
            drain(ar_a, PLANE - 1, 1)
            total = jnp.sum(ar_a[...], axis=0)
            pb_s[...] = total
            for k in range(1, N_Z):
                to_column(k, 1).start()
                to_column(k, 0).start()
            to_column(0, 0).start()
            ar_b[z_at] = total
            drain(ar_b, N_Z - 1, 3)

        @pl.when(core == 0)
        def _():
            drain(ar_b, N_Z, 3)

    sums = jnp.sum(ar_b[...], axis=0)
    dp_sum, dd_sum, rr_sum, pp_sum = [
        jnp.sum(jnp.where(at == i, sums, 0.0), axis=1, keepdims=True) for i in range(4)
    ]
    count = 1.0 / float(n_s * N_SPAN * ROWS * 625)
    coefficient = dp_sum * count
    beta = jnp.sqrt(
        (pp_sum - 2.0 * coefficient * dp_sum + coefficient * coefficient * dd_sum) * count
    )
    norm = jnp.sqrt(rr_sum * count)
    kry_ref[...] = jnp.where(at == 0, coefficient, jnp.where(at == 1, beta, norm))
    scale = 1.0 / beta
    for l in range(LAYERS):
        part = pl.ds(l * COLS, COLS)
        value = (x_out[1, part, :] - coefficient * x_s[1, part, :]) * scale
        bas_ref[:, l, :] = value[:, 0:625]

    @pl.when(core == 0)
    def _():
        drain(ar_a, PLANE // 2, 0)

    @pl.when(core == 1)
    def _():
        drain(ar_a, PLANE // 2 - 1, 0)
        drain(ar_a, 2 * N_Z - 1, 2)


def tail(res_in, bas_in, kry_in, res_out, bas_out, kry_out, sem):
    copies = [
        pltpu.make_async_copy(res_in, res_out, sem.at[0]),
        pltpu.make_async_copy(bas_in, bas_out, sem.at[1]),
    ]
    for copy in copies:
        copy.start()
    for i in range(3):
        kry_out[i] = jnp.sum(kry_in[0:1, i : i + 1])
    for copy in copies:
        copy.wait()


def local(state, direction, metric, face_source, send_rows):
    vmem = pl.BlockSpec(memory_space=pltpu.VMEM)
    hbm = pl.BlockSpec(memory_space=pltpu.HBM)
    shapes = [
        (state.shape, F32),
        (state.shape, F32),
        ((3, LAYERS, COLS), F32),
        ((4, COLS), jnp.int32),
        ((2, SLOTS), jnp.int32),
        ((384, 384), BF16),
        ((16, 128), F32),
        ((2, ROWS, 640), F32),
        ((10, ROWS, 128), F32),
        ((8 * ROWS, 128), F32),
        ((4, ROWS, 128), F32),
        ((3, ROWS, 128), F32),
        ((2, COLS, 128), F32),
        ((160, 160), BF16),
        ((160, 80), BF16),
        ((80, 160), BF16),
        ((LAYERS, 160, 256), F32),
        ((2, LAYERS, 2, COLS, 128), F32),
        ((2, LAYERS, 2, COLS, 128), F32),
        ((LAYERS, 80, 256), F32),
        ((LAYERS, 80, 256), F32),
        ((LAYERS, 80, 256), F32),
        ((LAYERS, 80, 256), F32),
        ((2, 2, COLS, 128), F32),
        ((2, 2, COLS, 128), F32),
        ((LAYERS, 160, 256), F32),
        ((8 * ROWS, 384), F32),
        ((3, 10, ROWS, 128), F32),
        ((3, 10, ROWS, 128), F32),
        ((3, 8, ROWS, 128), F32),
        ((3, 10 * ROWS, 128), F32),
        ((10 * ROWS, 128), F32),
        ((10, ROWS, 128), F32),
        ((10, ROWS, 128), F32),
        ((2, ROWS, 640), F32),
        ((4, CHUNK, 128), F32),
        ((1, 128), F32),
        ((1, 128), F32),
        ((PLANE, 1, 128), F32),
        ((N_Z, 1, 128), F32),
    ]
    res, bas, kry = pl.pallas_call(
        kernel,
        out_shape=(
            pltpu.VMEM(state.shape, F32),
            pltpu.VMEM(state.shape, F32),
            pltpu.VMEM((1, 128), F32),
        ),
        in_specs=[hbm] * 7,
        out_specs=(vmem, vmem, vmem),
        scratch_shapes=[pltpu.VMEM(shape, dtype) for shape, dtype in shapes]
        + [pltpu.SemaphoreType.DMA((n,)) for n in (12, 12, 4, 7)],
        compiler_params=pltpu.CompilerParams(
            collective_id=0, has_side_effects=True, vmem_limit_bytes=48 * 1024 * 1024
        ),
        name="hill",
    )(
        *[
            pltpu.with_memory_space_constraint(value, pltpu.HBM)
            for value in (
                state,
                direction,
                jnp.transpose(metric, (2, 1, 0)),
                jnp.transpose(face_source),
                send_rows[0],
                jnp.asarray(operator_table()),
                jnp.asarray(lane_table()),
            )
        ]
    )
    return pl.pallas_call(
        tail,
        out_shape=(
            pltpu.HBM(state.shape, F32),
            pltpu.HBM(state.shape, F32),
            jax.ShapeDtypeStruct((3,), F32),
        ),
        in_specs=[vmem] * 3,
        out_specs=(hbm, hbm, pl.BlockSpec(memory_space=pltpu.SMEM)),
        scratch_shapes=[pltpu.SemaphoreType.DMA((2,))],
        compiler_params=pltpu.CompilerParams(vmem_limit_bytes=1024 * 1024),
        name="tail",
    )(res, bas, kry)


def solution(mesh):
    in_specs = (
        P("stream", "span", None),
        P("stream", "span", None),
        P("stream", "span", None),
        P("stream", None),
        P("stream", None, None),
    )
    out_specs = (P("stream", "span", None), P("stream", "span", None), P())
    return jax.shard_map(local, mesh=mesh, in_specs=in_specs, out_specs=out_specs, check_vma=False)
```

```python
import math

import jax
import jax.numpy as jnp
import numpy as np
from jax import lax
from jax.experimental import pallas as pl
from jax.experimental.pallas import tpu as pltpu
from jax.sharding import PartitionSpec as P

MESH = pl.DeviceIdType.MESH
F32 = jnp.float32
BF16 = jnp.bfloat16

GAMMA = 1.4
VISC = 0.01
COND = VISC * GAMMA / ((GAMMA - 1.0) * 0.72)

COLS = 40
LAYERS = 2
ROWS = COLS * LAYERS
SLOTS = 33
SENT = 32
CHUNK = 8
STRIDES = (25, 5, 1)
XY_ROWS = 2 * 2 * SLOTS
Z_ROWS = 2 * 2 * COLS
N_X, N_Z, N_SPAN = 4, 8, 4
PLANE = 2 * N_X * N_SPAN
FAR_PLANE = sorted(
    ((i, j) for i in range(4) for j in range(4) if i or j),
    key=lambda step: -min(step[0], 4 - step[0]) - min(step[1], 4 - step[1]),
)
FAR_Z = (4, 3, 5, 2, 6, 1, 7)


def diff_table():
    spread = math.sqrt(3.0 / 7.0)
    points = np.array([-1.0, -spread, 0.0, spread, 1.0])
    weights = np.array(
        [
            np.prod([points[row_at] - points[other] for other in range(5) if other != row_at])
            for row_at in range(5)
        ]
    )
    matrix = np.zeros((5, 5))
    for row_at in range(5):
        for col_at in range(5):
            if row_at != col_at:
                matrix[row_at, col_at] = weights[row_at] / (
                    weights[col_at] * (points[row_at] - points[col_at])
                )
        matrix[row_at, row_at] = np.sum(
            [1.0 / (points[row_at] - points[other]) for other in range(5) if other != row_at]
        )
    return matrix


def operator_table():
    line = diff_table()
    line[0, 0] += 5.0
    line[4, 4] -= 5.0
    eye = np.eye(5)
    full = np.zeros((128, 384), np.float32)
    for axis in range(3):
        parts = [eye, eye, eye]
        parts[axis] = line
        volume = np.kron(np.kron(parts[0], parts[1]), parts[2])
        full[:125, axis * 128 : axis * 128 + 125] = volume.T
    high = full.astype(jnp.bfloat16)
    low = (full - high.astype(np.float32)).astype(jnp.bfloat16)
    return np.concatenate([high, high, low], axis=0)


def lane_table():
    table = np.zeros((16, 128), np.float32)
    lanes = np.arange(125)
    for axis, stride in enumerate(STRIDES):
        digit = (lanes // stride) % 5
        table[axis] = 9.0
        table[axis, :125] = digit
        table[3 + axis, :125] = 5.0 * (digit == 4) - 5.0 * (digit == 0)
        table[6 + axis] = 9.0
        for var in range(5):
            table[6 + axis, (lanes[digit == 4] + var * stride) % 128] = var
    return table


def roll(value, shift):
    shift %= 128
    return value if shift == 0 else pltpu.roll(value, shift, 1)


def split2(value):
    high = value.astype(BF16)
    return high, (value - high.astype(F32)).astype(BF16)


def split3(value):
    high = value.astype(BF16)
    rest = value - high.astype(F32)
    mid = rest.astype(BF16)
    return high, mid, (rest - mid.astype(F32)).astype(BF16)


def dot(a, b):
    return lax.dot_general(a, b, (((1,), (0,)), ((), ())), preferred_element_type=F32)


def primitive(u, du):
    r = 1.0 / u[0]
    v = [u[1 + i] * r for i in range(3)]
    dv = [(du[1 + i] - v[i] * du[0]) * r for i in range(3)]
    vm = u[1] * v[0] + u[2] * v[1] + u[3] * v[2]
    p = (GAMMA - 1.0) * (u[4] - 0.5 * vm)
    vdm = v[0] * du[1] + v[1] * du[2] + v[2] * du[3]
    vv = v[0] * v[0] + v[1] * v[1] + v[2] * v[2]
    dp = (GAMMA - 1.0) * (du[4] - vdm + 0.5 * vv * du[0])
    t = p * r
    dt = (dp - t * du[0]) * r
    s2 = vv + GAMMA * t
    ds2 = 2.0 * (v[0] * dv[0] + v[1] * dv[1] + v[2] * dv[2]) + GAMMA * dt
    return v, p, t, dv, dp, dt, s2, ds2


def inviscid(u, du, v, p, dv, dp, axis):
    flux = [u[1 + axis]]
    tangent = [du[1 + axis]]
    for i in range(3):
        f = u[1 + i] * v[axis]
        df = du[1 + i] * v[axis] + u[1 + i] * dv[axis]
        if i == axis:
            f = f + p
            df = df + dp
        flux.append(f)
        tangent.append(df)
    flux.append((u[4] + p) * v[axis])
    tangent.append((du[4] + dp) * v[axis] + (u[4] + p) * dv[axis])
    return flux, tangent


def stress(q):
    third = (2.0 / 3.0) * (q[0][0] + q[1][1] + q[2][2])
    tau = [[None] * 3 for _ in range(3)]
    for a in range(3):
        tau[a][a] = VISC * (2.0 * q[a][a] - third)
        for b in range(a + 1, 3):
            tau[a][b] = tau[b][a] = VISC * (q[a][b] + q[b][a])
    return tau


def kernel(
    state_in,
    dir_in,
    met_in,
    fs_in,
    sr_in,
    op_in,
    lane_in,
    res_ref,
    bas_ref,
    kry_ref,
    state_ref,
    dir_ref,
    met_ref,
    fs_ref,
    sr_ref,
    op_ref,
    lane_ref,
    x_s,
    u_s,
    w_s,
    c_s,
    m_s,
    fy_s,
    oo_s,
    or_s,
    so_s,
    tab_s,
    zp_s,
    zv_s,
    sb1,
    sb2,
    rx1,
    rx2,
    eb1,
    eb2,
    ex1,
    ex2,
    rz1,
    rz2,
    g_s,
    q_s,
    o_s,
    po_s,
    v_s,
    h_s,
    r_s,
    rs_s,
    y_s,
    x_out,
    acc_s,
    pt_s,
    pb_s,
    ar_a,
    ar_b,
    ruler,
    xs_send,
    xs_recv,
    sum_sem,
    in_sem,
):
    s = lax.axis_index("stream")
    p = lax.axis_index("span")
    n_s = 2 * N_X * N_Z
    s_lo, s_hi = lax.rem(s + n_s - 1, n_s), lax.rem(s + 1, n_s)
    p_lo, p_hi = lax.rem(p + N_SPAN - 1, N_SPAN), lax.rem(p + 1, N_SPAN)
    core = lax.rem(p, 2)
    x_at, z_at, y_hi, y_lo = s // (2 * N_Z), lax.rem(s // 2, N_Z), lax.rem(s, 2), p // 2
    y_at = 2 * y_hi + y_lo
    mine = 2 * (4 * x_at + y_at) + core

    def plane_peer(i, j, c):
        x, y = lax.rem(x_at + i, 4), lax.rem(y_at + j, 4)
        return {"stream": x * (2 * N_Z) + 2 * z_at + y // 2, "span": 2 * lax.rem(y, 2) + c}

    def column_peer(z, c):
        return {"stream": x_at * (2 * N_Z) + 2 * z + y_hi, "span": 2 * y_lo + c}

    barrier = pltpu.get_barrier_semaphore()

    def greet(target):
        pl.semaphore_signal(barrier, inc=1, device_id=target, device_id_type=MESH)

    greet({"stream": s_lo, "span": p})
    greet({"stream": s_hi, "span": p})
    greet({"stream": s, "span": p_lo})
    greet({"stream": s, "span": p_hi})

    loads = [
        pltpu.make_async_copy(src, dst, in_sem.at[i])
        for i, (src, dst) in enumerate(
            (
                (state_in, state_ref),
                (dir_in, dir_ref),
                (lane_in, lane_ref),
                (sr_in, sr_ref),
                (fs_in, fs_ref),
                (met_in, met_ref),
                (op_in, op_ref),
            )
        )
    ]
    for load in loads:
        load.start()


    for k in FAR_Z:
        greet(column_peer(lax.rem(z_at + k, N_Z), 1))

    @pl.when(core == 1)
    def _():
        for i, j in FAR_PLANE:
            greet(plane_peer(i, j, 0))
            greet(plane_peer(i, j, 1))
        greet(plane_peer(0, 0, 0))

    @pl.when(core == 0)
    def _():
        greet(column_peer(z_at, 1))

    for load in loads[:3]:
        load.wait()
    lane = lax.broadcasted_iota(jnp.int32, (CHUNK, 128), 1)
    rows = [jnp.broadcast_to(lane_ref[a : a + 1, :], (CHUNK, 128)) for a in range(9)]
    digit, sgn, over = rows[:3], rows[3:6], rows[6:]
    node = lane < 125

    for l in range(LAYERS):
        x_s[0, l * COLS : (l + 1) * COLS, 0:625] = state_ref[:, l, :]
        x_s[1, l * COLS : (l + 1) * COLS, 0:625] = dir_ref[:, l, :]

    def pack(fields, axis):
        stride = STRIDES[axis]
        lower = upper = fields[0]
        for v, field in enumerate(fields):
            if v:
                moved = roll(field, v * stride)
                lower = jnp.where(digit[axis] == float(v), moved, lower)
                upper = jnp.where(over[axis] == float(v), moved, upper)
        return lower, upper

    def settle(axis, up, value):
        return roll(value, (-4 if up else 4) * STRIDES[axis])

    def pack_axis(fields, axis, pt, l, rc, faces, settled):
        for up, value in enumerate(pack(fields, axis)):
            if settled:
                value = settle(axis, up, value)
            if axis < 2:
                at = (2 * axis + up) * COLS + rc
                tab_s[l, pl.ds(at, CHUNK), pt * 128 : pt * 128 + 128] = value
            else:
                faces[up, l, pt, pl.ds(rc, CHUNK), :] = value

    def layer_loop(body, l):
        def step(i, carry):
            rc = pl.multiple_of(i * CHUNK, CHUNK)
            body(l, rc, pl.multiple_of(l * COLS + rc, CHUNK))
            return carry

        lax.fori_loop(0, COLS // CHUNK, step, 0, unroll=COLS // CHUNK)

    def first(l, rc, row):
        for pt in range(2):
            tiles = [x_s[pt, pl.ds(row, CHUNK), 128 * t : 128 * t + 128] for t in range(5)]
            fields = []
            for v in range(5):
                value = roll(tiles[v], 3 * v)
                if v:
                    value = jnp.where(lane < 3 * v, roll(tiles[v - 1], 3 * v), value)
                idle = 1.0 if pt == 0 and v in (0, 4) else 0.0
                value = jnp.where(node, value, idle)
                u_s[pt * 5 + v, pl.ds(row, CHUNK), :] = value
                fields.append(value)
            for axis in range(3):
                pack_axis(fields, axis, pt, l, rc, zp_s, True)

    def remote(src, dst, sem, target):
        return pltpu.make_async_remote_copy(
            src_ref=src,
            dst_ref=dst,
            send_sem=xs_send.at[0],
            recv_sem=xs_recv.at[sem],
            device_id=target,
            device_id_type=MESH,
        )

    def drain(count, sem):
        part = ruler.at[pl.ds(0, count)]
        pltpu.make_async_copy(part, part, sem).wait()

    def z_copies(faces, rz, base):
        return [
            remote(faces.at[0, 0], rz.at[1], base, {"stream": s, "span": p_lo}),
            remote(faces.at[1, LAYERS - 1], rz.at[0], base, {"stream": s, "span": p_hi}),
        ]

    def xy_copies(sb, rx, eb, ex, l, base):
        lower, upper = pl.ds(0, SENT), pl.ds(COLS, SENT)
        below, above = {"stream": s_lo, "span": p}, {"stream": s_hi, "span": p}
        base += 1 + l
        return [
            remote(sb.at[l, lower], rx.at[l, upper], base, below),
            remote(sb.at[l, upper], rx.at[l, lower], base, above),
            remote(eb.at[l, 0], ex.at[l, 1], base, below),
            remote(eb.at[l, 1], ex.at[l, 0], base, above),
        ]

    def start(copies):
        for copy in copies:
            copy.start()

    def gather(hot, table):
        parts = split3(table)
        return dot(hot, parts[0]) + (dot(hot, parts[1]) + dot(hot, parts[2]))

    def fill(sb, eb, l):
        value = gather(so_s[...], tab_s[l])
        sb[l] = value
        eb[l, 0] = value[SENT:SLOTS]
        eb[l, 1] = value[COLS + SENT : COLS + SLOTS]

    with jax.named_scope("first0"):
        layer_loop(first, 0)

    for load in loads[3:]:
        load.wait()
    eye = lax.broadcasted_iota(jnp.int32, (COLS, COLS), 0) == lax.broadcasted_iota(
        jnp.int32, (COLS, COLS), 1
    )

    def column(row):
        return jnp.sum(
            jnp.where(eye, jnp.broadcast_to(row, (COLS, COLS)), 0.0), axis=1, keepdims=True
        )

    k_own = lax.broadcasted_iota(jnp.int32, (COLS, 160), 1)
    g_own = (
        jnp.where(k_own >= 40, 159, 0)
        + jnp.where(k_own >= 80, 159, 0)
        + jnp.where(k_own >= 120, 159, 0)
    )
    own_id = (4 * k_own - g_own).astype(F32)
    k_rec = lax.broadcasted_iota(jnp.int32, (COLS, 80), 1)
    rec_id = jnp.where(
        k_rec < SLOTS,
        k_rec + 160,
        jnp.where((k_rec >= COLS) & (k_rec < COLS + SLOTS), k_rec + 153, -5),
    ).astype(F32)
    slot = lax.broadcasted_iota(jnp.int32, (COLS, SLOTS), 0) == lax.broadcasted_iota(
        jnp.int32, (COLS, SLOTS), 1
    )
    for side in range(2):
        ids = sr_ref[side : side + 1, :].astype(F32)
        col = jnp.sum(
            jnp.where(slot, jnp.broadcast_to(ids, (COLS, SLOTS)), 0.0), axis=1, keepdims=True
        )
        so_s[side * COLS : (side + 1) * COLS, :] = jnp.where(col == own_id, 1.0, 0.0).astype(BF16)

    round1 = [xy_copies(sb1, rx1, eb1, ex1, l, 0) for l in range(LAYERS)]
    round1_z = z_copies(zp_s, rz1, 0)
    round2 = [xy_copies(sb2, rx2, eb2, ex2, l, 3) for l in range(LAYERS)]
    round2_z = z_copies(zv_s, rz2, 3)

    fill(sb1, eb1, 0)
    with jax.named_scope("first1"):
        layer_loop(first, 1)
        fill(sb1, eb1, 1)
    with jax.named_scope("barrier"):
        pl.semaphore_wait(barrier, 4 + 16 + 14 * core)
    start(round1_z)
    start(round1[0])
    start(round1[1])

    for f in range(4):
        col = column(fs_ref[f : f + 1, :].astype(F32))
        oo_s[f * COLS : (f + 1) * COLS, :] = jnp.where(col == own_id, 1.0, 0.0).astype(BF16)
        or_s[f * COLS : (f + 1) * COLS, :] = jnp.where(col == rec_id, 1.0, 0.0).astype(BF16)
        if f >= 2:
            fy_s[f - 2] = jnp.broadcast_to(col, (COLS, 128))
    for a in range(3):
        for l in range(LAYERS):
            m_s[a, l * COLS : (l + 1) * COLS, :] = jnp.broadcast_to(
                column(met_ref[a, l : l + 1, :]), (COLS, 128)
            )

    def own_gather(l):
        g_s[l] = gather(oo_s[...], tab_s[l])

    def far_gather(rx, ex, l):
        rx[l, SENT:SLOTS, :] = ex[l, 0]
        rx[l, COLS + SENT : COLS + SLOTS, :] = ex[l, 1]
        g_s[l] += gather(or_s[...], rx[l])

    for rx in (rx1, rx2):
        for l in range(LAYERS):
            for side in range(2):
                rx[l, side * COLS + SENT : (side + 1) * COLS, :] = jnp.zeros((COLS - SENT, 256), F32)

    def second(l, rc, row):
        u = [u_s[v, pl.ds(row, CHUNK), :] for v in range(10)]
        v, pr, t, dv, dp, dt, s2, ds2 = primitive(u[:5], u[5:])
        for i, value in enumerate(v + [t] + dv + [dt]):
            w_s[pl.ds(pl.multiple_of(i * ROWS + row, CHUNK), CHUNK), :] = value
        for i, value in enumerate([pr, dp, s2, ds2]):
            c_s[i, pl.ds(row, CHUNK), :] = value

    for l in range(LAYERS):
        layer_loop(second, l)
    high, low = split2(w_s[...])
    q_s[...] = dot(jnp.concatenate([high, low, high], axis=1), op_ref[...])
    for l in range(LAYERS):
        own_gather(l)

    def face_masks(rc):
        masks = []
        for axis in range(3):
            lower, upper = digit[axis] == 0.0, digit[axis] == 4.0
            if axis == 1:
                lower = lower & (fy_s[0, pl.ds(rc, CHUNK), :] >= 0.0)
                upper = upper & (fy_s[1, pl.ds(rc, CHUNK), :] >= 0.0)
            masks.append(lower | upper)
        return masks

    def packed_pair(axis, pt, l, rc, faces, rz):
        here = pl.ds(rc, CHUNK)
        if axis < 2:
            return [
                g_s[l, pl.ds(f * COLS + rc, CHUNK), pt * 128 : pt * 128 + 128]
                for f in (2 * axis, 2 * axis + 1)
            ]
        below = rz[0, pt, here, :] if l == 0 else faces[1, l - 1, pt, here, :]
        above = rz[1, pt, here, :] if l == LAYERS - 1 else faces[0, l + 1, pt, here, :]
        return [below, above]

    def unpack(pair, v, axis, masks, inside):
        mixed = jnp.where(digit[axis] == float(v), pair[0], pair[1])
        return jnp.where(masks[axis], roll(mixed, -v * STRIDES[axis]), inside)

    def third(l, rc, row):
        masks = face_masks(rc)
        here = pl.ds(row, CHUNK)
        u = [u_s[v, here, :] for v in range(10)]
        inside = [-value if v % 5 in (1, 2, 3) else value for v, value in enumerate(u)]
        q = [[], []]
        for axis in range(3):
            out = []
            for pt in range(2):
                pair = packed_pair(axis, pt, l, rc, zp_s, rz1)
                for v in range(5):
                    out.append(unpack(pair, v, axis, masks, inside[pt * 5 + v]))
            for i, value in enumerate(out):
                o_s[axis, i, here, :] = value
            v, pr, t, dv, dp, dt, s2, ds2 = primitive(out[:5], out[5:])
            for i, value in enumerate(v + [pr, s2] + dv + [dp, ds2]):
                po_s[axis, i, here, :] = value
            factor = m_s[axis, here, :]
            for i, value in enumerate(v + [t] + dv + [dt]):
                at = pl.multiple_of(i * ROWS + row, CHUNK)
                volume = q_s[pl.ds(at, CHUNK), axis * 128 : axis * 128 + 128]
                q[i // 4].append(factor * (volume + sgn[axis] * value))
        w = [w_s[pl.ds(pl.multiple_of(i * ROWS + row, CHUNK), CHUNK), :] for i in range(8)]
        tau, dtau = [stress([q[pt][4 * a : 4 * a + 3] for a in range(3)]) for pt in range(2)]
        for a in range(3):
            energy = COND * q[0][4 * a + 3]
            tangent = COND * q[1][4 * a + 3]
            for b in range(3):
                energy = energy + w[b] * tau[a][b]
                tangent = tangent + (w[4 + b] * tau[a][b] + w[b] * dtau[a][b])
            for pt, flux in enumerate((tau[a] + [energy], dtau[a] + [tangent])):
                for i, value in enumerate(flux):
                    v_s[a, pt * 4 + i, here, :] = value
                pack_axis(flux, a, pt, l, rc, zv_s, False)

    with jax.named_scope("wait1z"):
        drain(Z_ROWS, xs_recv.at[0])
    for l in range(LAYERS):
        with jax.named_scope("wait1"):
            drain(XY_ROWS, xs_recv.at[1 + l])
        with jax.named_scope("third"):
            far_gather(rx1, ex1, l)
            layer_loop(third, l)
            start(round2_z[l : l + 1])
            fill(sb2, eb2, l)
            start(round2[l])

    def fourth(l, rc, row):
        here = pl.ds(row, CHUNK)
        u = [u_s[v, here, :] for v in range(10)]
        w = [w_s[pl.ds(pl.multiple_of(i * ROWS + row, CHUNK), CHUNK), :] for i in range(8)]
        pr, dp, s2, ds2 = [c_s[i, here, :] for i in range(4)]
        total = [None] * 10
        for a in range(3):
            factor = m_s[a, here, :]
            flux, tangent = inviscid(u[:5], u[5:], w[:3], pr, w[4:7], dp, a)
            for pt, values in enumerate((flux, tangent)):
                for i, value in enumerate(values):
                    if i:
                        value = value - v_s[a, pt * 4 + i - 1, here, :]
                    at = pl.multiple_of((pt * 5 + i) * ROWS + row, CHUNK)
                    h_s[a, pl.ds(at, CHUNK), :] = factor * value
            out = [o_s[a, i, here, :] for i in range(10)]
            po = [po_s[a, i, here, :] for i in range(10)]
            flux, tangent = inviscid(out[:5], out[5:], po[:3], po[3], po[5:8], po[8], a)
            speed = jnp.sqrt(0.5 * (s2 + po[4]))
            dspeed = 0.25 * (ds2 + po[9]) / speed
            side = factor * sgn[a]
            drag = jnp.abs(side)
            for i in range(5):
                jump = out[i] - u[i]
                term = side * flux[i] - drag * (speed * jump)
                dterm = side * tangent[i] - drag * (dspeed * jump + speed * (out[5 + i] - u[5 + i]))
                total[i] = term if a == 0 else total[i] + term
                total[5 + i] = dterm if a == 0 else total[5 + i] + dterm
        for i in range(10):
            rs_s[i, here, :] = total[i]

    with jax.named_scope("fourth"):
        for l in range(LAYERS):
            own_gather(l)
            layer_loop(fourth, l)
    with jax.named_scope("resmm"):
        volume = None
        for a in range(3):
            high, low = split2(h_s[a])
            part = dot(jnp.concatenate([high, low, high], axis=1), op_ref[:, a * 128 : a * 128 + 128])
            volume = part if a == 0 else volume + part
        r_s[...] = volume
        acc_s[...] = jnp.zeros((4, CHUNK, 128), F32)

    def fifth(l, rc, row):
        masks = face_masks(rc)
        here = pl.ds(row, CHUNK)
        total = [
            r_s[pl.ds(pl.multiple_of(i * ROWS + row, CHUNK), CHUNK), :] + rs_s[i, here, :]
            for i in range(10)
        ]
        for a in range(3):
            side = m_s[a, here, :] * sgn[a]
            for pt in range(2):
                pair = packed_pair(a, pt, l, rc, zv_s, rz2)
                pair = [settle(a, 1, pair[0]), settle(a, 0, pair[1])]
                for i in range(4):
                    value = unpack(pair, i, a, masks, v_s[a, pt * 4 + i, here, :])
                    total[pt * 5 + 1 + i] = total[pt * 5 + 1 + i] - side * value
        total = [jnp.where(node, value, 0.0) for value in total]
        du = [u_s[5 + i, here, :] for i in range(5)]
        sums = [None] * 4
        for i in range(5):
            terms = (
                du[i] * total[5 + i],
                du[i] * du[i],
                total[i] * total[i],
                total[5 + i] * total[5 + i],
            )
            sums = [term if i == 0 else old + term for old, term in zip(sums, terms)]
        for i in range(4):
            acc_s[i] += sums[i]
        for i in range(10):
            y_s[i, here, :] = total[i]

    with jax.named_scope("wait2z"):
        drain(Z_ROWS, xs_recv.at[3])
    for l in range(LAYERS):
        with jax.named_scope("wait2"):
            drain(XY_ROWS, xs_recv.at[4 + l])
        with jax.named_scope("fifth"):
            far_gather(rx2, ex2, l)
            layer_loop(fifth, l)

    at = lax.broadcasted_iota(jnp.int32, (1, 128), 1)
    own = [jnp.sum(acc_s[i], axis=(0, 1), keepdims=True) for i in range(4)]
    own = jnp.where(at == 0, own[0], jnp.where(at == 1, own[1], jnp.where(at == 2, own[2], own[3])))
    pt_s[...] = own

    def to_plane(i, j):
        return pltpu.make_async_remote_copy(
            src_ref=pt_s,
            dst_ref=ar_a.at[mine],
            send_sem=sum_sem.at[0],
            recv_sem=sum_sem.at[1],
            device_id=plane_peer(i, j, 1),
            device_id_type=MESH,
        )

    def to_column(k, c):
        return pltpu.make_async_remote_copy(
            src_ref=pb_s,
            dst_ref=ar_b.at[z_at],
            send_sem=sum_sem.at[2],
            recv_sem=sum_sem.at[3],
            device_id=column_peer(lax.rem(z_at + k, N_Z), c),
            device_id_type=MESH,
        )

    for i, j in FAR_PLANE:
        to_plane(i, j).start()

    @pl.when(core == 0)
    def _():
        to_plane(0, 0).start()

    @pl.when(core == 1)
    def _():
        ar_a[mine] = own

    def tile(fields, t):
        value = roll(fields[t], -3 * t)
        if t < 4:
            value = jnp.where(lane < 125 - 3 * t, value, roll(fields[t + 1], 125 - 3 * t))
        return value

    def sixth(l, rc, row):
        here = pl.ds(row, CHUNK)
        fields = [y_s[i, here, :] for i in range(10)]
        for pt in range(2):
            for t in range(5):
                x_out[pt, here, 128 * t : 128 * t + 128] = tile(fields[5 * pt : 5 * pt + 5], t)

    with jax.named_scope("sixth"):
        for l in range(LAYERS):
            layer_loop(sixth, l)
        for l in range(LAYERS):
            res_ref[:, l, :] = x_out[0, l * COLS : (l + 1) * COLS, 0:625]

    with jax.named_scope("sums"):

        @pl.when(core == 1)
        def _():
            drain(PLANE - 1, sum_sem.at[1])
            total = jnp.sum(ar_a[...], axis=0)
            pb_s[...] = total
            for k in FAR_Z:
                to_column(k, 0).start()
                to_column(k, 1).start()
            to_column(0, 0).start()
            ar_b[z_at] = total
            drain(N_Z - 1, sum_sem.at[3])

        @pl.when(core == 0)
        def _():
            drain(N_Z, sum_sem.at[3])

    sums = jnp.sum(ar_b[...], axis=0)
    dp_sum, dd_sum, rr_sum, pp_sum = [
        jnp.sum(jnp.where(at == i, sums, 0.0), axis=1, keepdims=True) for i in range(4)
    ]
    count = 1.0 / float(n_s * N_SPAN * ROWS * 625)
    coefficient = dp_sum * count
    beta = jnp.sqrt(
        (pp_sum - 2.0 * coefficient * dp_sum + coefficient * coefficient * dd_sum) * count
    )
    norm = jnp.sqrt(rr_sum * count)
    kry_ref[...] = jnp.where(at == 0, coefficient, jnp.where(at == 1, beta, norm))
    scale = 1.0 / beta
    for l in range(LAYERS):
        part = pl.ds(l * COLS, COLS)
        value = (x_out[1, part, :] - coefficient * x_s[1, part, :]) * scale
        bas_ref[:, l, :] = value[:, 0:625]

    drain(2 * (LAYERS * XY_ROWS + Z_ROWS), xs_send.at[0])

    @pl.when(core == 0)
    def _():
        drain(PLANE // 2, sum_sem.at[0])

    @pl.when(core == 1)
    def _():
        drain(PLANE // 2 - 1, sum_sem.at[0])
        drain(2 * N_Z - 1, sum_sem.at[2])


def tail(res_in, bas_in, kry_in, res_out, bas_out, kry_out, kry_s, sem):
    kry_s[...] = kry_in[0, 0:3]
    copies = [
        pltpu.make_async_copy(kry_s, kry_out, sem.at[2]),
        pltpu.make_async_copy(res_in, res_out, sem.at[0]),
        pltpu.make_async_copy(bas_in, bas_out, sem.at[1]),
    ]
    for copy in copies:
        copy.start()
    for copy in copies:
        copy.wait()


def local(state, direction, metric, face_source, send_rows):
    vmem = pl.BlockSpec(memory_space=pltpu.VMEM)
    hbm = pl.BlockSpec(memory_space=pltpu.HBM)
    shapes = [
        (state.shape, F32),
        (state.shape, F32),
        ((3, LAYERS, COLS), F32),
        ((4, COLS), jnp.int32),
        ((2, SLOTS), jnp.int32),
        ((384, 384), BF16),
        ((16, 128), F32),
        ((2, ROWS, 640), F32),
        ((10, ROWS, 128), F32),
        ((8 * ROWS, 128), F32),
        ((4, ROWS, 128), F32),
        ((3, ROWS, 128), F32),
        ((2, COLS, 128), F32),
        ((160, 160), BF16),
        ((160, 80), BF16),
        ((80, 160), BF16),
        ((LAYERS, 160, 256), F32),
        ((2, LAYERS, 2, COLS, 128), F32),
        ((2, LAYERS, 2, COLS, 128), F32),
        ((LAYERS, 80, 256), F32),
        ((LAYERS, 80, 256), F32),
        ((LAYERS, 80, 256), F32),
        ((LAYERS, 80, 256), F32),
        ((LAYERS, 2, 1, 256), F32),
        ((LAYERS, 2, 1, 256), F32),
        ((LAYERS, 2, 1, 256), F32),
        ((LAYERS, 2, 1, 256), F32),
        ((2, 2, COLS, 128), F32),
        ((2, 2, COLS, 128), F32),
        ((LAYERS, 160, 256), F32),
        ((8 * ROWS, 384), F32),
        ((3, 10, ROWS, 128), F32),
        ((3, 10, ROWS, 128), F32),
        ((3, 8, ROWS, 128), F32),
        ((3, 10 * ROWS, 128), F32),
        ((10 * ROWS, 128), F32),
        ((10, ROWS, 128), F32),
        ((10, ROWS, 128), F32),
        ((2, ROWS, 640), F32),
        ((4, CHUNK, 128), F32),
        ((1, 128), F32),
        ((1, 128), F32),
        ((PLANE, 1, 128), F32),
        ((N_Z, 1, 128), F32),
        ((2 * (LAYERS * XY_ROWS + Z_ROWS), 1, 128), F32),
    ]
    res, bas, kry = pl.pallas_call(
        kernel,
        out_shape=(
            pltpu.VMEM(state.shape, F32),
            pltpu.VMEM(state.shape, F32),
            pltpu.VMEM((1, 128), F32),
        ),
        in_specs=[hbm] * 7,
        out_specs=(vmem, vmem, vmem),
        scratch_shapes=[pltpu.VMEM(shape, dtype) for shape, dtype in shapes]
        + [pltpu.SemaphoreType.DMA((n,)) for n in (1, 6, 4, 7)],
        compiler_params=pltpu.CompilerParams(
            collective_id=0, has_side_effects=True, vmem_limit_bytes=48 * 1024 * 1024
        ),
        name="hill",
    )(
        *[
            pltpu.with_memory_space_constraint(value, pltpu.HBM)
            for value in (
                state,
                direction,
                jnp.transpose(metric, (2, 1, 0)),
                jnp.transpose(face_source),
                send_rows[0],
                jnp.asarray(operator_table()),
                jnp.asarray(lane_table()),
            )
        ]
    )
    return pl.pallas_call(
        tail,
        out_shape=(
            pltpu.HBM(state.shape, F32),
            pltpu.HBM(state.shape, F32),
            pltpu.HBM((3,), F32),
        ),
        in_specs=[vmem] * 3,
        out_specs=(hbm, hbm, hbm),
        scratch_shapes=[pltpu.VMEM((3,), F32), pltpu.SemaphoreType.DMA((3,))],
        compiler_params=pltpu.CompilerParams(vmem_limit_bytes=1024 * 1024),
        name="tail",
    )(res, bas, kry)


def solution(mesh):
    in_specs = (
        P("stream", "span", None),
        P("stream", "span", None),
        P("stream", "span", None),
        P("stream", None),
        P("stream", None, None),
    )
    out_specs = (P("stream", "span", None), P("stream", "span", None), P())
    return jax.shard_map(local, mesh=mesh, in_specs=in_specs, out_specs=out_specs, check_vma=False)
```
